128 devices in a mesh: dp: 1, tp: 128 (over z, y, x, core).
Axes of the slice: x: 4, y: 4, z: 4, core: 2. Of those that a mesh axis runs over, the one named last changes fastest.
Arguments:
- hidden: bfloat16 [4096, 1152], P(('dp', 'tp'))
- w_head: bfloat16 [1152, 262144], P(None, 'tp')
- labels: int32 [4096], P(('dp', 'tp'))
Outputs:
- output 1: float32 [1], P('dp')
- output 2: bfloat16 [4096, 1152], P(('dp', 'tp'))
- output 3: bfloat16 [1152, 262144], P('dp', 'tp')
All inputs are finite; a program needn't handle non-finite values.
Results may differ from the reference program's by a relative error of at most 0.001.
Values are sent between devices in bfloat16 or wider.
A program may use at most 1 GiB of HBM per device.

```python
import math
import jax
import jax.numpy as jnp
from jax import lax

HIDDEN = 1152
VOCAB = 262144
TOKENS = 4096

ROW_BLOCK = math.gcd(TOKENS, 64)


def setup_inputs(seed: int = 0, part: int = 0) -> dict:
    base_key = jax.random.key(seed)
    key_w, key_parts = jax.random.split(base_key)
    key_x, key_lab = jax.random.split(jax.random.fold_in(key_parts, part))
    w_head = jax.random.normal(key_w, (HIDDEN, VOCAB), jnp.float32) * HIDDEN ** -0.5
    labels = jax.random.randint(key_lab, (TOKENS,), 0, VOCAB, dtype=jnp.int32)
    label_boost = math.log(VOCAB) - 1.0
    noise_x = jax.random.normal(key_x, (TOKENS, HIDDEN), jnp.float32)
    hidden = noise_x + label_boost * jnp.take(w_head, labels, axis=1).T
    return {"hidden": hidden.astype(jnp.bfloat16), "w_head": w_head.astype(jnp.bfloat16), "labels": labels}


def reference(hidden, w_head, labels):
    inv_tokens = 1.0 / TOKENS
    num_blocks = TOKENS // ROW_BLOCK
    hid_blocks = hidden.reshape(num_blocks, ROW_BLOCK, HIDDEN)
    lab_blocks = labels.reshape(num_blocks, ROW_BLOCK)
    vocab_ids = jnp.arange(VOCAB, dtype=jnp.int32)
    w_trans = w_head.T

    def row_step(acc_dw, block):
        hid_blk, lab_blk = block
        logits = jnp.dot(hid_blk, w_head, preferred_element_type=jnp.float32)
        row_max = jnp.max(logits, axis=1, keepdims=True)
        shifted = jnp.exp(logits - row_max)
        row_sum = jnp.sum(shifted, axis=1, keepdims=True)
        onehot = (vocab_ids[None, :] == lab_blk[:, None]).astype(jnp.float32)
        target = jnp.sum(logits * onehot, axis=1)
        token_loss = row_max[:, 0] + jnp.log(row_sum[:, 0]) - target
        grad_out = ((shifted / row_sum - onehot) * inv_tokens).astype(jnp.bfloat16)
        acc_dw = acc_dw + jnp.dot(hid_blk.T, grad_out, preferred_element_type=jnp.float32)
        dx_blk = jnp.dot(grad_out, w_trans, preferred_element_type=jnp.float32)
        return acc_dw, (token_loss, dx_blk.astype(jnp.bfloat16))

    zero_dw = jnp.zeros((HIDDEN, VOCAB), jnp.float32)
    acc_dw, (losses, dx_blocks) = lax.scan(row_step, zero_dw, (hid_blocks, lab_blocks))
    mean_loss = (jnp.sum(losses) * inv_tokens).reshape(1)
    return mean_loss, dx_blocks.reshape(TOKENS, HIDDEN), acc_dw.astype(jnp.bfloat16)
```

```python
import functools

import jax
import jax.numpy as jnp
from jax import lax
from jax.experimental import pallas as pl
from jax.experimental.pallas import tpu as pltpu
from jax.sharding import PartitionSpec as P

MESH = pl.DeviceIdType.MESH
F32 = jnp.float32
BF16 = jnp.bfloat16

SIDE = 4
STRIDES = (32, 8, 2)
ORDERS = ((2, 1, 0), (1, 0, 2), (0, 2, 1))
SLABS = 2
ROWS = 16
BLOCK = 256
HID = 1152
COLOUR = HID // 3
HALF = 2048
TOKENS = 4096
INV = 1.0 / TOKENS
LANES = 128


def body(x_hbm, w_hbm, lab_hbm,
         loss_ref, dhid_ref, dhead_hbm, p_hbm, hrecv_hbm,
         x_ref, w_ref, g_ref, dx_ref, buf_ref, r1_ref, r2_ref, r3_ref,
         labrow_ref, lab_ref, m_ref, s_ref, t_ref, scale_ref, srow_ref, st_ref, fin_ref, lossx_ref,
         ag_send, ag_recv, lab_send, lab_recv, w_send, w_recv, st_send, st_recv, rs_send, rs_recv,
         hd_send, hd_recv, ls_send, ls_recv, in_sem, p_sem, g_sem, h_sem, out_sem):
    me = lax.axis_index("tp")
    core = lax.rem(me, 2)
    chip = lax.div(me, 2)
    coords = (lax.div(chip, 16), lax.rem(lax.div(chip, 4), 4), lax.rem(chip, 4))
    partner = me + 1 - 2 * core

    def ring(axis, d):
        return lax.rem(coords[axis] + d, SIDE)

    def rank(axis, d):
        return me + (ring(axis, d) - coords[axis]) * STRIDES[axis]

    def remote(src, dst, send, recv, target):
        return pltpu.make_async_remote_copy(src_ref=src, dst_ref=dst, send_sem=send, recv_sem=recv,
                                            device_id={"tp": target}, device_id_type=MESH)

    def cols(c):
        return pl.ds(COLOUR * c, COLOUR)

    own = []
    for s in range(SLABS):
        own.append(pltpu.make_async_copy(x_hbm.at[pl.ds(ROWS * s, ROWS)],
                                         x_ref.at[(s,) + coords], in_sem.at[s]))
    own.append(pltpu.make_async_copy(lab_hbm, labrow_ref.at[coords], in_sem.at[2]))
    w_own = pltpu.make_async_copy(w_hbm, w_ref.at[core], in_sem.at[3])
    for copy in own:
        copy.start()
    w_own.start()

    barrier = pltpu.get_barrier_semaphore()
    peers = [partner] + [rank(a, d) for a in range(3) for d in (1, 2, 3)]
    for peer in peers:
        pl.semaphore_signal(barrier, inc=1, device_id={"tp": peer}, device_id_type=MESH)
    pl.semaphore_wait(barrier, len(peers))

    def ag_copy(s, phase, c, d):
        order = ORDERS[c]
        idx = list(coords)
        for a in order[:phase]:
            idx[a] = slice(None)
        view = x_ref.at[(s,) + tuple(idx) + (slice(None), cols(c))]
        return remote(view, view, ag_send.at[s, phase, c, d - 1], ag_recv.at[s, phase, c, d - 1],
                      rank(order[phase], d))

    def ag_start(s, phase):
        for d in (2, 1, 3):
            for c in range(3):
                ag_copy(s, phase, c, d).start()

    def ag_wait(s, phase):
        for d in (1, 2, 3):
            for c in range(3):
                ag_copy(s, phase, c, d).wait_recv()

    def lab_copy(phase, d):
        order = ORDERS[0]
        idx = list(coords)
        for a in order[:phase]:
            idx[a] = slice(None)
        view = labrow_ref.at[tuple(idx)]
        return remote(view, view, lab_send.at[phase, d - 1], lab_recv.at[phase, d - 1], rank(order[phase], d))

    def lab_start(phase):
        for d in (1, 2, 3):
            lab_copy(phase, d).start()

    def lab_wait(phase):
        for d in (1, 2, 3):
            lab_copy(phase, d).wait_recv()

    for copy in own:
        copy.wait()
    lab_start(0)
    ag_start(0, 0)
    ag_start(1, 0)
    w_copy = remote(w_hbm, w_ref.at[core], w_send, w_recv, partner)
    w_copy.start()
    lab_wait(0)
    lab_start(1)
    ag_wait(0, 0)
    ag_start(0, 1)
    ag_wait(1, 0)
    ag_start(1, 1)
    lab_wait(1)
    lab_start(2)
    ag_wait(0, 1)
    ag_start(0, 2)
    ag_wait(1, 1)
    ag_start(1, 2)
    lab_wait(2)

    lane16 = lax.broadcasted_iota(jnp.int32, (ROWS, LANES), 1)
    row16 = lax.broadcasted_iota(jnp.int32, (ROWS, LANES), 0)
    first_col = chip * (2 * HALF)

    def spread(k, carry):
        kz, ky, kx = lax.div(k, 16), lax.rem(lax.div(k, 4), 4), lax.rem(k, 4)
        row = jnp.broadcast_to(labrow_ref[kz, ky, kx], (ROWS, LANES)).astype(F32)
        for s in range(SLABS):
            col = jnp.sum(jnp.where(lane16 == row16 + ROWS * s, row, 0.0), axis=1, keepdims=True)
            lab_ref[s, k] = jnp.broadcast_to(col, (ROWS, LANES)).astype(jnp.int32) - first_col - lane16
        return carry

    lax.fori_loop(0, 64, spread, 0, unroll=4)

    def p_copy(n, slot):
        return pltpu.make_async_copy(buf_ref.at[slot, pl.ds(0, 1024)], p_hbm.at[n], p_sem.at[slot])

    def g_load(n, slot):
        return pltpu.make_async_copy(p_hbm.at[n], buf_ref.at[slot, pl.ds(0, 1024)], g_sem.at[slot])

    def st_copy(s, axis, d):
        view = st_ref.at[s, axis, coords[axis]]
        return remote(view, view, st_send.at[s, axis, d - 1], st_recv.at[s, axis, d - 1], rank(axis, d))

    def st_start(s, axis):
        for d in (2, 1, 3):
            st_copy(s, axis, d).start()

    def st_merge(s, axis):
        for d in (1, 2, 3):
            st_copy(s, axis, d).wait_recv()
        top = st_ref[s, axis, 0, 0]
        for i in range(1, SIDE):
            top = jnp.maximum(top, st_ref[s, axis, i, 0])
        total = jnp.zeros_like(top)
        target = jnp.zeros_like(top)
        for i in range(SIDE):
            total += st_ref[s, axis, i, 1] * jnp.exp(st_ref[s, axis, i, 0] - top)
            target += st_ref[s, axis, i, 2]
        if axis < 2:
            here = coords[axis + 1]
            st_ref[s, axis + 1, here, 0] = top
            st_ref[s, axis + 1, here, 1] = total
            st_ref[s, axis + 1, here, 2] = target
            st_start(s, axis + 1)
        else:
            fin_ref[s, 0] = top
            fin_ref[s, 1] = INV / total
            fin_ref[s, 2] = top + jnp.log(total) - target

    def logits_block(s, b):
        n = s * SIDE + b
        slot = lax.rem(n, 2)

        @pl.when(n >= 2)
        def _():
            p_copy(n - 2, slot).wait()

        xb = x_ref[s, b].reshape(BLOCK, HID)
        for q in range(4):
            buf_ref[slot, pl.ds(q * BLOCK, BLOCK), :] = jnp.dot(
                xb, w_ref[q // 2, :, (q % 2) * 1024:(q % 2 + 1) * 1024], preferred_element_type=F32)

        def rows(i, carry):
            r0 = pl.multiple_of(i * 8, 8)
            lab = lab_ref[s, b * 16 + lax.div(i, 2), pl.ds(pl.multiple_of(lax.rem(i, 2) * 8, 8), 8), :]
            z = [buf_ref[slot, pl.ds(pl.multiple_of(q * BLOCK + r0, 8), 8), l * LANES:(l + 1) * LANES]
                 for q in range(4) for l in range(8)]
            tops = z
            while len(tops) > 1:
                tops = [jnp.maximum(tops[k], tops[k + 1]) for k in range(0, len(tops), 2)]
            top = tops[0]
            sums = [jnp.zeros((8, LANES), F32) for _ in range(2)]
            tgt = [jnp.zeros((8, LANES), F32) for _ in range(2)]
            for k in range(32):
                p = jnp.exp(z[k] - top)
                q, l = k // 8, k % 8
                buf_ref[slot, pl.ds(pl.multiple_of(q * BLOCK + r0, 8), 8), l * LANES:(l + 1) * LANES] = p
                sums[k % 2] += p
                tgt[k % 2] = jnp.where(lab == k * LANES, z[k], tgt[k % 2])
            m_ref[s, pl.ds(pl.multiple_of(b * BLOCK + r0, 8), 8), :] = top
            s_ref[pl.ds(r0, 8), :] = sums[0] + sums[1]
            t_ref[pl.ds(r0, 8), :] = tgt[0] + tgt[1]
            return carry

        lax.fori_loop(0, BLOCK // 8, rows, 0, unroll=2)
        p_copy(n, slot).start()
        for i in range(2):
            m_t = m_ref[s, pl.ds(pl.multiple_of(b * BLOCK + i * LANES, LANES), LANES), :].T
            s_t = s_ref[i * LANES:(i + 1) * LANES, :].T
            t_t = t_ref[i * LANES:(i + 1) * LANES, :].T
            top = jnp.max(m_t, axis=0, keepdims=True)
            at = pl.ds(b * 2 + i, 1)
            srow_ref[0, at, :] = top
            srow_ref[1, at, :] = jnp.sum(s_t * jnp.exp(m_t - top), axis=0, keepdims=True)
            srow_ref[2, at, :] = jnp.sum(t_t, axis=0, keepdims=True)

    def st_begin(s):
        for k in range(3):
            st_ref[s, 0, coords[0], k] = srow_ref[k]
        st_start(s, 0)

    def rs_copy(s, phase, c, d):
        order = ORDERS[c]
        idx = [slice(None)] * 3
        for a in order[:phase]:
            idx[a] = coords[a]
        idx[order[phase]] = ring(order[phase], d)
        land = (r1_ref, r2_ref, r3_ref)[phase]
        return remote(dx_ref.at[(s,) + tuple(idx) + (slice(None), cols(c))], land.at[s, c, d - 1],
                      rs_send.at[s, phase, c, d - 1], rs_recv.at[s, phase, c, d - 1], rank(order[phase], d))

    def rs_start(s, phase):
        for d in (2, 1, 3):
            for c in range(3):
                rs_copy(s, phase, c, d).start()

    def rs_add(s, phase):
        for c in range(3):
            for d in (1, 2, 3):
                rs_copy(s, phase, c, d).wait_recv()
            order = ORDERS[c]
            sl = slice(c * COLOUR, (c + 1) * COLOUR)
            idx = [None] * 3
            for a in order[:phase + 1]:
                idx[a] = coords[a]
            free = [a for a in range(3) if idx[a] is None]
            if phase == 0:
                def add(i, carry):
                    for j in range(SIDE):
                        at = list(idx)
                        at[free[0]], at[free[1]] = i, j
                        at = (s,) + tuple(at)
                        dx_ref[at + (slice(None), sl)] = (
                            (dx_ref[at + (slice(None), sl)] + r1_ref[s, c, 0, i, j])
                            + (r1_ref[s, c, 1, i, j] + r1_ref[s, c, 2, i, j]))
                    return carry
                lax.fori_loop(0, SIDE, add, 0)
            elif phase == 1:
                def add(i, carry):
                    at = list(idx)
                    at[free[0]] = i
                    at = (s,) + tuple(at)
                    dx_ref[at + (slice(None), sl)] = (
                        (dx_ref[at + (slice(None), sl)] + r2_ref[s, c, 0, i])
                        + (r2_ref[s, c, 1, i] + r2_ref[s, c, 2, i]))
                    return carry
                lax.fori_loop(0, SIDE, add, 0)
            else:
                total = ((dx_ref[(s,) + tuple(idx) + (slice(None), sl)] + r3_ref[s, c, 0])
                         + (r3_ref[s, c, 1] + r3_ref[s, c, 2]))
                dhid_ref[s * ROWS:(s + 1) * ROWS, sl] = total.astype(BF16)
        if phase < 2:
            rs_start(s, phase + 1)

    def grad_block(s, b):
        n = s * SIDE + b
        slot = lax.rem(n, 2)

        @pl.when(n < 2 * SIDE - 1)
        def _():
            g_load(n + 1, 1 - slot).start()

        for i in range(2):
            at = pl.ds(b * 2 + i, 1)
            top = jnp.broadcast_to(fin_ref[s, 0, at, :], (LANES, LANES)).T
            inv = jnp.broadcast_to(fin_ref[s, 1, at, :], (LANES, LANES)).T
            m = m_ref[s, pl.ds(pl.multiple_of(b * BLOCK + i * LANES, LANES), LANES), :]
            scale_ref[i * LANES:(i + 1) * LANES, :] = jnp.exp(m - top) * inv
        g_load(n, slot).wait()

        def rows(i, carry):
            r0 = pl.multiple_of(i * ROWS, ROWS)
            lab = lab_ref[s, b * 16 + i]
            scale = scale_ref[pl.ds(r0, ROWS), :]
            out_row = pl.multiple_of(n * BLOCK + r0, ROWS)
            for k in range(32):
                q, l = k // 8, k % 8
                p = buf_ref[slot, pl.ds(pl.multiple_of(q * BLOCK + r0, 8), ROWS), l * LANES:(l + 1) * LANES]
                g = p * scale - jnp.where(lab == k * LANES, INV, 0.0)
                g_ref[k // 16, pl.ds(out_row, ROWS), (k % 16) * LANES:(k % 16 + 1) * LANES] = g.astype(BF16)
            return carry

        lax.fori_loop(0, BLOCK // ROWS, rows, 0, unroll=2)
        at = pl.ds(pl.multiple_of(n * BLOCK, BLOCK), BLOCK)
        nt = (((1,), (1,)), ((), ()))
        dx = (lax.dot_general(g_ref[0, at, :], w_ref[0], nt, preferred_element_type=F32)
              + lax.dot_general(g_ref[1, at, :], w_ref[1], nt, preferred_element_type=F32))
        dx_ref[s, b] = dx.reshape(SIDE, SIDE, ROWS, HID)

    w_own.wait()
    w_copy.wait_recv()
    ag_wait(0, 2)

    def logits_first(b, carry):
        logits_block(0, b)
        return carry

    lax.fori_loop(0, SIDE, logits_first, 0)
    st_begin(0)
    ag_wait(1, 2)

    def logits_second(b, carry):
        logits_block(1, b)
        for axis in range(3):
            pl.when(b == axis)(functools.partial(st_merge, 0, axis))
        return carry

    lax.fori_loop(0, SIDE, logits_second, 0)
    st_begin(1)
    p_copy(6, 0).wait()
    p_copy(7, 1).wait()
    g_load(0, 0).start()

    def grad_first(b, carry):
        grad_block(0, b)
        for axis in range(3):
            pl.when(b == axis)(functools.partial(st_merge, 1, axis))
        return carry

    lax.fori_loop(0, SIDE, grad_first, 0)
    rs_start(0, 0)

    lossx_ref[core] = fin_ref[0, 2] + fin_ref[1, 2]
    ls_copy = remote(lossx_ref.at[core], lossx_ref.at[core], ls_send, ls_recv, partner)
    ls_copy.start()

    def grad_second(b, carry):
        grad_block(1, b)
        return carry

    lax.fori_loop(0, SIDE, grad_second, 0)
    rs_start(1, 0)
    ls_copy.wait_recv()
    loss_ref[...] = jnp.broadcast_to(jnp.sum(lossx_ref[0] + lossx_ref[1]) * INV, (8, LANES))

    def flip(k, carry):
        kz, ky = lax.div(lax.rem(k, 8), 2), lax.rem(k, 2) * 2
        xs = x_ref[lax.div(k, 8), kz, pl.ds(ky, 2)].reshape(LANES, HID)
        w_ref[1, :, pl.ds(pl.multiple_of(k * LANES, LANES), LANES)] = xs.T
        return carry

    lax.fori_loop(0, 2 * 1024 // LANES, flip, 0)

    def area(k):
        return buf_ref.at[k // 2, :, pl.ds((k % 2) * 512, 512)]

    def head_copy(j, slot):
        return remote(buf_ref.at[0, :, pl.ds(pl.multiple_of(slot * 512, 512), 512)], hrecv_hbm.at[j],
                      hd_send.at[slot], hd_recv.at[j], partner)

    def head_load(j, slot):
        return pltpu.make_async_copy(hrecv_hbm.at[j], buf_ref.at[1, :, pl.ds(pl.multiple_of(slot * 512, 512), 512)],
                                     h_sem.at[slot])

    def head_dot(h, j):
        return jnp.dot(w_ref[1], g_ref[h, :, pl.ds(pl.multiple_of(j * 512, 512), 512)],
                       preferred_element_type=F32)

    def theirs(j, carry):
        slot = lax.rem(j, 2)

        @pl.when(j >= 2)
        def _():
            head_copy(j - 2, slot).wait_send()

        buf_ref[0, :, pl.ds(pl.multiple_of(slot * 512, 512), 512)] = head_dot(1 - core, j)
        head_copy(j, slot).start()
        pl.when(j == 2)(functools.partial(rs_add, 0, 0))
        return carry

    lax.fori_loop(0, 4, theirs, 0)
    head_copy(2, 0).wait_send()
    head_copy(3, 1).wait_send()

    def out_copy(j):
        at = pl.ds(pl.multiple_of(j * 512, 512), 512)
        return pltpu.make_async_copy(w_ref.at[0, :, at], dhead_hbm.at[:, at], out_sem.at[j])

    def ours(j, carry):
        slot = lax.rem(j, 2)
        head_copy(j, 0).wait_recv()
        head_load(j, slot).start()
        at = pl.ds(pl.multiple_of(j * 512, 512), 512)
        buf_ref[0, :, pl.ds(pl.multiple_of(slot * 512, 512), 512)] = head_dot(core, j)
        head_load(j, slot).wait()

        def add(i, c2):
            r = pl.ds(pl.multiple_of(i * 16, 16), 16)
            w_ref[0, r, at] = (buf_ref[0, r, pl.ds(pl.multiple_of(slot * 512, 512), 512)]
                               + buf_ref[1, r, pl.ds(pl.multiple_of(slot * 512, 512), 512)]).astype(BF16)
            return c2

        lax.fori_loop(0, HID // 16, add, 0, unroll=4)
        out_copy(j).start()
        pl.when(j == 2)(functools.partial(rs_add, 1, 0))
        pl.when(j == 3)(functools.partial(rs_add, 0, 1))
        return carry

    lax.fori_loop(0, 4, ours, 0)
    rs_add(1, 1)
    rs_add(0, 2)
    rs_add(1, 2)

    for j in range(4):
        out_copy(j).wait()
    w_copy.wait_send()
    ls_copy.wait_send()
    for phase in range(3):
        for d in (1, 2, 3):
            lab_copy(phase, d).wait_send()
            for s in range(SLABS):
                st_copy(s, phase, d).wait_send()
                for c in range(3):
                    ag_copy(s, phase, c, d).wait_send()
                    rs_copy(s, phase, c, d).wait_send()


def solution(mesh):
    any_space = pl.BlockSpec(memory_space=pl.ANY)
    vmem = pl.BlockSpec(memory_space=pltpu.VMEM)
    dma = pltpu.SemaphoreType.DMA

    def local_step(hid_loc, w_loc, lab_loc):
        labels = jnp.pad(lab_loc.reshape(1, -1), ((0, 0), (0, LANES - lab_loc.shape[0])))
        flops = 3 * 2 * TOKENS * HID * HALF
        loss, d_hidden, d_head, _, _ = pl.pallas_call(
            body,
            out_shape=(
                jax.ShapeDtypeStruct((8, LANES), F32),
                jax.ShapeDtypeStruct((SLABS * ROWS, HID), BF16),
                jax.ShapeDtypeStruct((HID, HALF), BF16),
                jax.ShapeDtypeStruct((8, 1024, 1024), F32),
                jax.ShapeDtypeStruct((4, HID, 512), F32),
            ),
            in_specs=[any_space, any_space, any_space],
            out_specs=(vmem, vmem, any_space, any_space, any_space),
            scratch_shapes=[
                pltpu.VMEM((SLABS, SIDE, SIDE, SIDE, ROWS, HID), BF16),
                pltpu.VMEM((2, HID, HALF), BF16),
                pltpu.VMEM((2, 2048, HALF), BF16),
                pltpu.VMEM((SLABS, SIDE, SIDE, SIDE, ROWS, HID), F32),
                pltpu.VMEM((2, HID, 1024), F32),
                pltpu.VMEM((SLABS, 3, 3, SIDE, SIDE, ROWS, COLOUR), F32),
                pltpu.VMEM((SLABS, 3, 3, SIDE, ROWS, COLOUR), F32),
                pltpu.VMEM((SLABS, 3, 3, ROWS, COLOUR), F32),
                pltpu.VMEM((SIDE, SIDE, SIDE, 1, LANES), jnp.int32),
                pltpu.VMEM((SLABS, 64, ROWS, LANES), jnp.int32),
                pltpu.VMEM((SLABS, 1024, LANES), F32),
                pltpu.VMEM((BLOCK, LANES), F32),
                pltpu.VMEM((BLOCK, LANES), F32),
                pltpu.VMEM((BLOCK, LANES), F32),
                pltpu.VMEM((3, 8, LANES), F32),
                pltpu.VMEM((SLABS, 3, SIDE, 3, 8, LANES), F32),
                pltpu.VMEM((SLABS, 3, 8, LANES), F32),
                pltpu.VMEM((2, 8, LANES), F32),
                dma((SLABS, 3, 3, 3)), dma((SLABS, 3, 3, 3)),
                dma((3, 3)), dma((3, 3)),
                dma, dma,
                dma((SLABS, 3, 3)), dma((SLABS, 3, 3)),
                dma((SLABS, 3, 3, 3)), dma((SLABS, 3, 3, 3)),
                dma((2,)), dma((4,)),
                dma, dma,
                dma((4,)), dma((2,)), dma((2,)), dma((2,)), dma((4,)),
            ],
            compiler_params=pltpu.CompilerParams(
                collective_id=0, has_side_effects=True, vmem_limit_bytes=67043328),
            cost_estimate=pl.CostEstimate(flops=flops, bytes_accessed=100_000_000, transcendentals=TOKENS * HALF),
        )(hid_loc, w_loc, labels)
        return loss[0, :1], d_hidden, d_head

    return jax.shard_map(
        local_step,
        mesh=mesh,
        in_specs=(P(("dp", "tp"), None), P(None, "tp"), P(("dp", "tp"))),
        out_specs=(P("dp"), P(("dp", "tp"), None), P("dp", "tp")),
        check_vma=False,
    )
```

```python
import functools

import jax
import jax.numpy as jnp
from jax import lax
from jax.experimental import pallas as pl
from jax.experimental.pallas import tpu as pltpu
from jax.sharding import PartitionSpec as P

MESH = pl.DeviceIdType.MESH
F32 = jnp.float32
BF16 = jnp.bfloat16

SIDE = 4
STRIDES = (32, 8, 2)
ORDERS = ((2, 1, 0), (1, 0, 2), (0, 2, 1))
SLABS = 2
ROWS = 16
BLOCK = 256
HID = 1152
COLOUR = HID // 3
HALF = 2048
TOKENS = 4096
INV = 1.0 / TOKENS
LANES = 128


def body(x_hbm, w_hbm, lab_hbm,
         loss_ref, dhid_ref, dhead_hbm, p_hbm, hrecv_hbm,
         x_ref, w_ref, g_ref, dx_ref, buf_ref, r1_ref, r2_ref, r3_ref,
         labown_ref, labrow_ref, lab_ref, m_ref, s_ref, t_ref, scale_ref, srow_ref, st_ref, fin_ref, lossx_ref,
         ag_send, ag_recv, lab_send, lab_recv, w_send, w_recv, st_send, st_recv, rs_send, rs_recv, r1_send, r1_recv,
         hd_send, hd_recv, ls_send, ls_recv, in_sem, p_sem, g_sem, h_sem, out_sem):
    me = lax.axis_index("tp")
    core = lax.rem(me, 2)
    chip = lax.div(me, 2)
    coords = (lax.div(chip, 16), lax.rem(lax.div(chip, 4), 4), lax.rem(chip, 4))
    partner = me + 1 - 2 * core

    def ring(axis, d):
        return lax.rem(coords[axis] + d, SIDE)

    def rank(axis, d):
        return me + (ring(axis, d) - coords[axis]) * STRIDES[axis]

    def remote(src, dst, send, recv, target):
        return pltpu.make_async_remote_copy(src_ref=src, dst_ref=dst, send_sem=send, recv_sem=recv,
                                            device_id={"tp": target}, device_id_type=MESH)

    def cols(c):
        return pl.ds(COLOUR * c, COLOUR)

    own = []
    for s in range(SLABS):
        own.append(pltpu.make_async_copy(x_hbm.at[pl.ds(ROWS * s, ROWS)],
                                         x_ref.at[(s,) + coords], in_sem.at[s]))
    own.append(pltpu.make_async_copy(lab_hbm, labown_ref, in_sem.at[2]))
    w_own = pltpu.make_async_copy(w_hbm, w_ref.at[core], in_sem.at[3])
    for copy in own:
        copy.start()
    w_own.start()

    with jax.named_scope("meet"):
        barrier = pltpu.get_barrier_semaphore()
        peers = [partner] + [rank(a, d) for a in range(3) for d in (1, 2, 3)]
        for peer in peers:
            pl.semaphore_signal(barrier, inc=1, device_id={"tp": peer}, device_id_type=MESH)
        pl.semaphore_wait(barrier, len(peers))

    def ag_copy(s, phase, c, d):
        order = ORDERS[c]
        idx = list(coords)
        for a in order[:phase]:
            idx[a] = slice(None)
        view = x_ref.at[(s,) + tuple(idx) + (slice(None), cols(c))]
        return remote(view, view, ag_send.at[s, phase, c, d - 1], ag_recv.at[s, phase, c, d - 1],
                      rank(order[phase], d))

    def ag_start(s, phase):
        for d in (2, 1, 3):
            for c in range(3):
                ag_copy(s, phase, c, d).start()

    def ag_wait(s, phase):
        for d in (1, 2, 3):
            for c in range(3):
                ag_copy(s, phase, c, d).wait_recv()

    def lab_copy(phase, d):
        order = ORDERS[0]
        idx = list(coords)
        for a in order[:phase]:
            idx[a] = slice(None)
        view = labrow_ref.at[tuple(idx)]
        return remote(view, view, lab_send.at[phase, d - 1], lab_recv.at[phase, d - 1], rank(order[phase], d))

    def lab_start(phase):
        for d in (1, 2, 3):
            lab_copy(phase, d).start()

    def lab_wait(phase):
        for d in (1, 2, 3):
            lab_copy(phase, d).wait_recv()

    with jax.named_scope("ag"):
        for copy in own:
            copy.wait()
        labrow_ref[coords + (slice(None), slice(0, SLABS * ROWS))] = labown_ref[...]
        ag_start(0, 0)
        w_copy = remote(w_hbm, w_ref.at[core], w_send, w_recv, partner)
        w_copy.start()
        lab_start(0)
        ag_wait(0, 0)
        ag_start(0, 1)
        ag_start(1, 0)
        lab_wait(0)
        lab_start(1)
        ag_wait(0, 1)
        lab_wait(1)
        lab_start(2)
        ag_start(0, 2)
        ag_wait(1, 0)
        ag_start(1, 1)
        lab_wait(2)

    lane16 = lax.broadcasted_iota(jnp.int32, (ROWS, LANES), 1)
    row16 = lax.broadcasted_iota(jnp.int32, (ROWS, LANES), 0)
    first_col = chip * (2 * HALF)

    def spread(k, carry):
        kz, ky, kx = lax.div(k, 16), lax.rem(lax.div(k, 4), 4), lax.rem(k, 4)
        row = jnp.broadcast_to(labrow_ref[kz, ky, kx], (ROWS, LANES)).astype(F32)
        for s in range(SLABS):
            col = jnp.sum(jnp.where(lane16 == row16 + ROWS * s, row, 0.0), axis=1, keepdims=True)
            lab_ref[s, k] = jnp.broadcast_to(col, (ROWS, LANES)).astype(jnp.int32) - first_col - lane16
        return carry

    with jax.named_scope("spread"):
        lax.fori_loop(0, 64, spread, 0, unroll=4)

    def p_copy(n, slot):
        return pltpu.make_async_copy(buf_ref.at[slot, pl.ds(0, 1024)], p_hbm.at[n], p_sem.at[slot])

    def plane(k):
        return lax.rem(coords[0] + k + 1, SIDE)

    def g_load(t):
        slot = lax.rem(t, 2)
        n = lax.div(t, SIDE) * SIDE + plane(lax.rem(t, SIDE))
        return pltpu.make_async_copy(p_hbm.at[n], buf_ref.at[slot, pl.ds(0, 1024)], g_sem.at[slot])

    def st_copy(s, axis, d):
        view = st_ref.at[s, axis, coords[axis]]
        return remote(view, view, st_send.at[s, axis, d - 1], st_recv.at[s, axis, d - 1], rank(axis, d))

    def st_start(s, axis):
        for d in (2, 1, 3):
            st_copy(s, axis, d).start()

    def st_merge(s, axis):
        with jax.named_scope("st_wait"):
            for d in (1, 2, 3):
                st_copy(s, axis, d).wait_recv()
        top = st_ref[s, axis, 0, 0]
        for i in range(1, SIDE):
            top = jnp.maximum(top, st_ref[s, axis, i, 0])
        total = jnp.zeros_like(top)
        target = jnp.zeros_like(top)
        for i in range(SIDE):
            total += st_ref[s, axis, i, 1] * jnp.exp(st_ref[s, axis, i, 0] - top)
            target += st_ref[s, axis, i, 2]
        if axis < 2:
            here = coords[axis + 1]
            st_ref[s, axis + 1, here, 0] = top
            st_ref[s, axis + 1, here, 1] = total
            st_ref[s, axis + 1, here, 2] = target
            st_start(s, axis + 1)
        else:
            fin_ref[s, 0] = top
            fin_ref[s, 1] = INV / total
            fin_ref[s, 2] = top + jnp.log(total) - target

    def logits_block(s, b):
        n = s * SIDE + b
        slot = lax.rem(n, 2)

        @pl.when(n >= 2)
        def _():
            p_copy(n - 2, slot).wait()

        with jax.named_scope("z_dot"):
            xb = x_ref[s, b].reshape(BLOCK, HID)
            for q in range(4):
                buf_ref[slot, pl.ds(q * BLOCK, BLOCK), :] = jnp.dot(
                    xb, w_ref[q // 2, :, (q % 2) * 1024:(q % 2 + 1) * 1024], preferred_element_type=F32)

        @pl.when(n == 0)
        def _():
            ag_wait(1, 1)
            ag_start(1, 2)

        @pl.when(n == 2 * SIDE - 1)
        def _():
            p_copy(2 * SIDE - 2, 0).wait()
            g_load(0).start()

        def rows(i, carry):
            r0 = pl.multiple_of(i * 8, 8)
            lab = lab_ref[s, b * 16 + lax.div(i, 2), pl.ds(pl.multiple_of(lax.rem(i, 2) * 8, 8), 8), :]
            z = [buf_ref[slot, pl.ds(pl.multiple_of(q * BLOCK + r0, 8), 8), l * LANES:(l + 1) * LANES]
                 for q in range(4) for l in range(8)]
            tops = z
            while len(tops) > 1:
                tops = [jnp.maximum(tops[k], tops[k + 1]) for k in range(0, len(tops), 2)]
            top = tops[0]
            sums = [jnp.zeros((8, LANES), F32) for _ in range(2)]
            tgt = [jnp.zeros((8, LANES), F32) for _ in range(2)]
            for k in range(32):
                p = jnp.exp(z[k] - top)
                q, l = k // 8, k % 8
                buf_ref[slot, pl.ds(pl.multiple_of(q * BLOCK + r0, 8), 8), l * LANES:(l + 1) * LANES] = p
                sums[k % 2] += p
                tgt[k % 2] = jnp.where(lab == k * LANES, z[k], tgt[k % 2])
            m_ref[s, pl.ds(pl.multiple_of(b * BLOCK + r0, 8), 8), :] = top
            s_ref[pl.ds(r0, 8), :] = sums[0] + sums[1]
            t_ref[pl.ds(r0, 8), :] = tgt[0] + tgt[1]
            return carry

        with jax.named_scope("z_rows"):
            lax.fori_loop(0, BLOCK // 8, rows, 0, unroll=2)
        p_copy(n, slot).start()
        with jax.named_scope("z_stat"):
            for i in range(2):
                m_t = m_ref[s, pl.ds(pl.multiple_of(b * BLOCK + i * LANES, LANES), LANES), :].T
                s_t = s_ref[i * LANES:(i + 1) * LANES, :].T
                t_t = t_ref[i * LANES:(i + 1) * LANES, :].T
                top = jnp.max(m_t, axis=0, keepdims=True)
                at = pl.ds(b * 2 + i, 1)
                srow_ref[0, at, :] = top
                srow_ref[1, at, :] = jnp.sum(s_t * jnp.exp(m_t - top), axis=0, keepdims=True)
                srow_ref[2, at, :] = jnp.sum(t_t, axis=0, keepdims=True)

    def st_begin(s):
        for k in range(3):
            st_ref[s, 0, coords[0], k] = srow_ref[k]
        st_start(s, 0)

    def rs_copy(s, phase, c, d):
        order = ORDERS[c]
        idx = [slice(None)] * 3
        for a in order[:phase]:
            idx[a] = coords[a]
        idx[order[phase]] = ring(order[phase], d)
        land = (r1_ref, r2_ref, r3_ref)[phase]
        return remote(dx_ref.at[(s,) + tuple(idx) + (slice(None), cols(c))], land.at[s, c, d - 1],
                      rs_send.at[s, phase, c, d - 1], rs_recv.at[s, phase, c, d - 1], rank(order[phase], d))

    def rs_plane(s, k, c, d):
        axis = ORDERS[c][0]
        b = plane(k)
        idx = [b, slice(None), slice(None)]
        if axis:
            idx[axis] = ring(axis, d)
        return remote(dx_ref.at[(s,) + tuple(idx) + (slice(None), cols(c))], r1_ref.at[s, c, d - 1, b],
                      r1_send.at[s, c, k, d - 1], r1_recv.at[s, c, k, d - 1], rank(axis, d))

    def rs_line(s, k):
        b = plane(k)
        return remote(dx_ref.at[s, b, :, :, :, cols(2)], r1_ref.at[s, 2, k],
                      rs_send.at[s, 0, 2, k], rs_recv.at[s, 0, 2, k], rank(0, k + 1))

    def rs_first(s, k):
        for d in (2, 1, 3):
            for c in range(2):
                rs_plane(s, k, c, d).start()

        @pl.when(k < SIDE - 1)
        def _():
            rs_line(s, k).start()

    def rs_start(s, phase):
        for d in (2, 1, 3):
            for c in range(3):
                rs_copy(s, phase, c, d).start()

    def rs_add(s, phase):
        for c in range(3):
            with jax.named_scope("rs_wait"):
                for d in (1, 2, 3):
                    if phase:
                        rs_copy(s, phase, c, d).wait_recv()
                    elif c == 2:
                        rs_line(s, d - 1).wait_recv()
                    else:
                        for k in range(SIDE):
                            rs_plane(s, k, c, d).wait_recv()
            order = ORDERS[c]
            sl = slice(c * COLOUR, (c + 1) * COLOUR)
            idx = [None] * 3
            for a in order[:phase + 1]:
                idx[a] = coords[a]
            free = [a for a in range(3) if idx[a] is None]
            if phase == 0:
                def add(i, carry):
                    for j in range(SIDE):
                        at = list(idx)
                        at[free[0]], at[free[1]] = i, j
                        at = (s,) + tuple(at)
                        dx_ref[at + (slice(None), sl)] = (
                            (dx_ref[at + (slice(None), sl)] + r1_ref[s, c, 0, i, j])
                            + (r1_ref[s, c, 1, i, j] + r1_ref[s, c, 2, i, j]))
                    return carry
                lax.fori_loop(0, SIDE, add, 0)
            elif phase == 1:
                def add(i, carry):
                    at = list(idx)
                    at[free[0]] = i
                    at = (s,) + tuple(at)
                    dx_ref[at + (slice(None), sl)] = (
                        (dx_ref[at + (slice(None), sl)] + r2_ref[s, c, 0, i])
                        + (r2_ref[s, c, 1, i] + r2_ref[s, c, 2, i]))
                    return carry
                lax.fori_loop(0, SIDE, add, 0)
            else:
                total = ((dx_ref[(s,) + tuple(idx) + (slice(None), sl)] + r3_ref[s, c, 0])
                         + (r3_ref[s, c, 1] + r3_ref[s, c, 2]))
                dhid_ref[s * ROWS:(s + 1) * ROWS, sl] = total.astype(BF16)
        if phase < 2:
            rs_start(s, phase + 1)

    def grad_block(s, k):
        b = plane(k)
        n = s * SIDE + b
        t = s * SIDE + k
        slot = lax.rem(t, 2)

        @pl.when(t < 2 * SIDE - 1)
        def _():
            g_load(t + 1).start()

        with jax.named_scope("g_scale"):
            for i in range(2):
                at = pl.ds(b * 2 + i, 1)
                top = jnp.broadcast_to(fin_ref[s, 0, at, :], (LANES, LANES)).T
                inv = jnp.broadcast_to(fin_ref[s, 1, at, :], (LANES, LANES)).T
                m = m_ref[s, pl.ds(pl.multiple_of(b * BLOCK + i * LANES, LANES), LANES), :]
                scale_ref[i * LANES:(i + 1) * LANES, :] = jnp.exp(m - top) * inv
        g_load(t).wait()

        def rows(i, carry):
            r0 = pl.multiple_of(i * ROWS, ROWS)
            lab = lab_ref[s, b * 16 + i]
            scale = scale_ref[pl.ds(r0, ROWS), :]
            out_row = pl.multiple_of(n * BLOCK + r0, ROWS)
            for k in range(32):
                q, l = k // 8, k % 8
                p = buf_ref[slot, pl.ds(pl.multiple_of(q * BLOCK + r0, 8), ROWS), l * LANES:(l + 1) * LANES]
                g = p * scale - jnp.where(lab == k * LANES, INV, 0.0)
                g_ref[k // 16, pl.ds(out_row, ROWS), (k % 16) * LANES:(k % 16 + 1) * LANES] = g.astype(BF16)
            return carry

        with jax.named_scope("g_rows"):
            lax.fori_loop(0, BLOCK // ROWS, rows, 0, unroll=2)
        at = pl.ds(pl.multiple_of(n * BLOCK, BLOCK), BLOCK)
        nt = (((1,), (1,)), ((), ()))
        with jax.named_scope("dx_dot"):
            dx = (lax.dot_general(g_ref[0, at, :], w_ref[0], nt, preferred_element_type=F32)
                  + lax.dot_general(g_ref[1, at, :], w_ref[1], nt, preferred_element_type=F32))
            dx_ref[s, b] = dx.reshape(SIDE, SIDE, ROWS, HID)
        rs_first(s, k)

    with jax.named_scope("first_wait"):
        w_own.wait()
        w_copy.wait_recv()
        ag_wait(0, 2)

    def logits_first(b, carry):
        logits_block(0, b)
        return carry

    lax.fori_loop(0, SIDE, logits_first, 0)
    st_begin(0)
    with jax.named_scope("second_wait"):
        ag_wait(1, 2)

    def logits_second(b, carry):
        logits_block(1, b)
        for axis in range(3):
            pl.when(b == axis)(functools.partial(st_merge, 0, axis))
        return carry

    lax.fori_loop(0, SIDE, logits_second, 0)
    st_begin(1)
    p_copy(7, 1).wait()

    def grad_first(b, carry):
        grad_block(0, b)
        for axis in range(3):
            pl.when(b == axis)(functools.partial(st_merge, 1, axis))
        return carry

    lax.fori_loop(0, SIDE, grad_first, 0)

    lossx_ref[core] = fin_ref[0, 2] + fin_ref[1, 2]
    ls_copy = remote(lossx_ref.at[core], lossx_ref.at[core], ls_send, ls_recv, partner)
    ls_copy.start()

    def grad_second(b, carry):
        grad_block(1, b)
        pl.when(b == 2)(functools.partial(rs_add, 0, 0))
        return carry

    lax.fori_loop(0, SIDE, grad_second, 0)
    ls_copy.wait_recv()
    loss_ref[0] = jnp.sum(lossx_ref[0] + lossx_ref[1]) * INV

    def flip(k, carry):
        kz, ky = lax.div(lax.rem(k, 8), 2), lax.rem(k, 2) * 2
        xs = x_ref[lax.div(k, 8), kz, pl.ds(ky, 2)].reshape(LANES, HID)
        w_ref[1, :, pl.ds(pl.multiple_of(k * LANES, LANES), LANES)] = xs.T
        return carry

    with jax.named_scope("flip"):
        lax.fori_loop(0, 2 * 1024 // LANES, flip, 0)

    def half(slot):
        return pl.ds(pl.multiple_of(slot * 512, 512), 512)

    def head_copy(j):
        slot = lax.rem(j, 2)
        return remote(buf_ref.at[0, :, half(slot)], hrecv_hbm.at[j], hd_send.at[slot], hd_recv.at[j], partner)

    def head_load(j):
        return pltpu.make_async_copy(hrecv_hbm.at[j], buf_ref.at[1, :, pl.ds(512, 512)], h_sem)

    def head_dot(h, j):
        with jax.named_scope("h_dot"):
            return jnp.dot(w_ref[1], g_ref[h, :, half(j)], preferred_element_type=F32)

    def out_copy(j):
        return pltpu.make_async_copy(w_ref.at[0, :, half(j)], dhead_hbm.at[:, half(j)], out_sem.at[j])

    def theirs(j):
        @pl.when(jnp.int32(j) >= 2)
        def _():
            head_copy(j - 2).wait_send()

        buf_ref[0, :, half(lax.rem(j, 2))] = head_dot(1 - core, j)
        head_copy(j).start()

    def ours(j):
        with jax.named_scope("h_wait"):
            head_copy(j).wait_recv()
        head_load(j).start()
        buf_ref[1, :, pl.ds(0, 512)] = head_dot(core, j)
        with jax.named_scope("h_load"):
            head_load(j).wait()

        def add(i, carry):
            r = pl.ds(pl.multiple_of(i * 16, 16), 16)
            w_ref[0, r, half(j)] = (buf_ref[1, r, pl.ds(0, 512)] + buf_ref[1, r, pl.ds(512, 512)]).astype(BF16)
            return carry

        with jax.named_scope("h_add"):
            lax.fori_loop(0, HID // 16, add, 0, unroll=4)
        out_copy(j).start()

    def pair(r, carry):
        theirs(r + 1)
        pl.when(r == 0)(functools.partial(rs_add, 0, 1))
        pl.when(r == 1)(functools.partial(rs_add, 0, 2))
        ours(r)
        pl.when(r == 0)(functools.partial(rs_add, 1, 0))
        pl.when(r == 1)(functools.partial(rs_add, 1, 1))
        return carry

    theirs(0)
    lax.fori_loop(0, 3, pair, 0)
    rs_add(1, 2)
    ours(3)
    head_copy(2).wait_send()
    head_copy(3).wait_send()

    with jax.named_scope("tail"):
        for j in range(4):
            out_copy(j).wait()
        w_copy.wait_send()
        ls_copy.wait_send()
        for phase in range(3):
            for d in (1, 2, 3):
                lab_copy(phase, d).wait_send()
                for s in range(SLABS):
                    st_copy(s, phase, d).wait_send()
                    for c in range(3):
                        ag_copy(s, phase, c, d).wait_send()
                        if phase:
                            rs_copy(s, phase, c, d).wait_send()
        for s in range(SLABS):
            for d in (1, 2, 3):
                rs_line(s, d - 1).wait_send()
                for k in range(SIDE):
                    for c in range(2):
                        rs_plane(s, k, c, d).wait_send()


PIECES = 8


def hand_out(loss_in, dhid_in, dhead_in, loss_out, dhid_out, dhead_out, dhid_v, dhead_v, in_sem, out_sem):
    ways = [(dhid_in, dhid_v, dhid_out)]
    for i in range(PIECES):
        at = pl.ds(i * (HID // PIECES), HID // PIECES)
        ways.append((dhead_in.at[at], dhead_v.at[at], dhead_out.at[at]))
    ins = [pltpu.make_async_copy(a, v, in_sem.at[i]) for i, (a, v, _) in enumerate(ways)]
    outs = [pltpu.make_async_copy(v, o, out_sem.at[i]) for i, (_, v, o) in enumerate(ways)]
    for copy in ins:
        copy.start()
    loss_out[0] = loss_in[0]
    for here, there in zip(ins, outs):
        here.wait()
        there.start()
    for copy in outs:
        copy.wait()


def solution(mesh):
    any_space = pl.BlockSpec(memory_space=pl.ANY)
    vmem = pl.BlockSpec(memory_space=pltpu.VMEM)
    smem = pl.BlockSpec(memory_space=pltpu.SMEM)
    dma = pltpu.SemaphoreType.DMA

    def local_step(hid_loc, w_loc, lab_loc):
        labels = lab_loc.reshape(1, -1)
        flops = 3 * 2 * TOKENS * HID * HALF
        loss, d_hidden, d_head, _, _ = pl.pallas_call(
            body,
            out_shape=(
                jax.ShapeDtypeStruct((1,), F32),
                jax.ShapeDtypeStruct((SLABS * ROWS, HID), BF16),
                jax.ShapeDtypeStruct((HID, HALF), BF16),
                jax.ShapeDtypeStruct((8, 1024, 1024), F32),
                jax.ShapeDtypeStruct((4, HID, 512), F32),
            ),
            in_specs=[any_space, any_space, any_space],
            out_specs=(smem, vmem, any_space, any_space, any_space),
            scratch_shapes=[
                pltpu.VMEM((SLABS, SIDE, SIDE, SIDE, ROWS, HID), BF16),
                pltpu.VMEM((2, HID, HALF), BF16),
                pltpu.VMEM((2, 2048, HALF), BF16),
                pltpu.VMEM((SLABS, SIDE, SIDE, SIDE, ROWS, HID), F32),
                pltpu.VMEM((2, HID, 1024), F32),
                pltpu.VMEM((SLABS, 3, 3, SIDE, SIDE, ROWS, COLOUR), F32),
                pltpu.VMEM((SLABS, 3, 3, SIDE, ROWS, COLOUR), F32),
                pltpu.VMEM((SLABS, 3, 3, ROWS, COLOUR), F32),
                pltpu.VMEM((1, SLABS * ROWS), jnp.int32),
                pltpu.VMEM((SIDE, SIDE, SIDE, 1, LANES), jnp.int32),
                pltpu.VMEM((SLABS, 64, ROWS, LANES), jnp.int32),
                pltpu.VMEM((SLABS, 1024, LANES), F32),
                pltpu.VMEM((BLOCK, LANES), F32),
                pltpu.VMEM((BLOCK, LANES), F32),
                pltpu.VMEM((BLOCK, LANES), F32),
                pltpu.VMEM((3, 8, LANES), F32),
                pltpu.VMEM((SLABS, 3, SIDE, 3, 8, LANES), F32),
                pltpu.VMEM((SLABS, 3, 8, LANES), F32),
                pltpu.VMEM((2, 8, LANES), F32),
                dma((SLABS, 3, 3, 3)), dma((SLABS, 3, 3, 3)),
                dma((3, 3)), dma((3, 3)),
                dma, dma,
                dma((SLABS, 3, 3)), dma((SLABS, 3, 3)),
                dma((SLABS, 3, 3, 3)), dma((SLABS, 3, 3, 3)), dma((SLABS, 2, SIDE, 3)), dma((SLABS, 2, SIDE, 3)),
                dma((2,)), dma((4,)),
                dma, dma,
                dma((4,)), dma((2,)), dma((2,)), dma, dma((4,)),
            ],
            compiler_params=pltpu.CompilerParams(
                collective_id=0, has_side_effects=True, vmem_limit_bytes=67043328),
            cost_estimate=pl.CostEstimate(flops=flops, bytes_accessed=100_000_000, transcendentals=TOKENS * HALF),
        )(hid_loc, w_loc, labels)
        return pl.pallas_call(
            hand_out,
            out_shape=(
                jax.ShapeDtypeStruct((1,), F32),
                jax.ShapeDtypeStruct((SLABS * ROWS, HID), BF16),
                jax.ShapeDtypeStruct((HID, HALF), BF16),
            ),
            in_specs=[smem, any_space, any_space],
            out_specs=(smem, any_space, any_space),
            scratch_shapes=[
                pltpu.VMEM((SLABS * ROWS, HID), BF16),
                pltpu.VMEM((HID, HALF), BF16),
                dma((PIECES + 1,)), dma((PIECES + 1,)),
            ],
        )(loss, d_hidden, d_head)

    return jax.shard_map(
        local_step,
        mesh=mesh,
        in_specs=(P(("dp", "tp"), None), P(None, "tp"), P(("dp", "tp"))),
        out_specs=(P("dp"), P(("dp", "tp"), None), P("dp", "tp")),
        check_vma=False,
    )
```

```python
import functools

import jax
import jax.numpy as jnp
from jax import lax
from jax.experimental import pallas as pl
from jax.experimental.pallas import tpu as pltpu
from jax.sharding import PartitionSpec as P

MESH = pl.DeviceIdType.MESH
F32 = jnp.float32
BF16 = jnp.bfloat16

SIDE = 4
STRIDES = (32, 8, 2)
ORDERS = ((2, 1, 0), (1, 0, 2), (0, 2, 1))
SLABS = 2
ROWS = 16
BLOCK = 256
HID = 1152
COLOUR = HID // 3
HALF = 2048
TOKENS = 4096
INV = 1.0 / TOKENS
LANES = 128


def body(x_hbm, w_hbm, lab_hbm,
         loss_ref, dhid_ref, dhead_hbm, p_hbm, hrecv_hbm,
         x_ref, w_ref, g_ref, dx_ref, buf_ref, r1_ref, r2_ref, r3_ref,
         labown_ref, labrow_ref, lab_ref, m_ref, s_ref, t_ref, scale_ref, srow_ref, st_ref, fin_ref, lossx_ref,
         ag_send, ag_recv, lab_send, lab_recv, w_send, w_recv, st_send, st_recv, rs_send, rs_recv,
         hd_send, hd_recv, ls_send, ls_recv, in_sem, p_sem, g_sem, h_sem, out_sem):
    me = lax.axis_index("tp")
    core = lax.rem(me, 2)
    chip = lax.div(me, 2)
    coords = (lax.div(chip, 16), lax.rem(lax.div(chip, 4), 4), lax.rem(chip, 4))
    partner = me + 1 - 2 * core

    def ring(axis, d):
        return lax.rem(coords[axis] + d, SIDE)

    def rank(axis, d):
        return me + (ring(axis, d) - coords[axis]) * STRIDES[axis]

    def remote(src, dst, send, recv, target):
        return pltpu.make_async_remote_copy(src_ref=src, dst_ref=dst, send_sem=send, recv_sem=recv,
                                            device_id={"tp": target}, device_id_type=MESH)

    def cols(c):
        return pl.ds(COLOUR * c, COLOUR)

    own = []
    for s in range(SLABS):
        own.append(pltpu.make_async_copy(x_hbm.at[pl.ds(ROWS * s, ROWS)],
                                         x_ref.at[(s,) + coords], in_sem.at[s]))
    own.append(pltpu.make_async_copy(lab_hbm, labown_ref, in_sem.at[2]))
    w_own = pltpu.make_async_copy(w_hbm, w_ref.at[core], in_sem.at[3])
    for copy in own:
        copy.start()
    w_own.start()

    with jax.named_scope("meet"):
        barrier = pltpu.get_barrier_semaphore()
        peers = [partner] + [rank(a, d) for a in range(3) for d in (1, 2, 3)]
        for peer in peers:
            pl.semaphore_signal(barrier, inc=1, device_id={"tp": peer}, device_id_type=MESH)
        pl.semaphore_wait(barrier, len(peers))

    def ag_copy(s, phase, c, d):
        order = ORDERS[c]
        idx = list(coords)
        for a in order[:phase]:
            idx[a] = slice(None)
        view = x_ref.at[(s,) + tuple(idx) + (slice(None), cols(c))]
        return remote(view, view, ag_send.at[s, phase], ag_recv.at[s, phase],
                      rank(order[phase], d))

    def ag_start(s, phase):
        for d in (2, 1, 3):
            for c in range(3):
                ag_copy(s, phase, c, d).start()

    def ag_all(s, phase):
        view = (x_ref.at[s, 0, 0, pl.ds(0, 3)], x_ref.at[s, 0, pl.ds(0, 3)], x_ref.at[s, pl.ds(0, 3)])[phase]
        return remote(view, view, ag_send.at[s, phase], ag_recv.at[s, phase], partner)

    def ag_wait(s, phase):
        ag_all(s, phase).wait_recv()

    def lab_copy(phase, d):
        order = ORDERS[0]
        idx = list(coords)
        for a in order[:phase]:
            idx[a] = slice(None)
        view = labrow_ref.at[tuple(idx)]
        return remote(view, view, lab_send.at[phase], lab_recv.at[phase], rank(order[phase], d))

    def lab_start(phase):
        for d in (1, 2, 3):
            lab_copy(phase, d).start()

    def lab_all(phase):
        view = (labrow_ref.at[0, 0, pl.ds(0, 3)], labrow_ref.at[0, pl.ds(0, 3)], labrow_ref.at[pl.ds(0, 3)])[phase]
        return remote(view, view, lab_send.at[phase], lab_recv.at[phase], partner)

    def lab_wait(phase):
        lab_all(phase).wait_recv()

    with jax.named_scope("ag"):
        for copy in own:
            copy.wait()
        labrow_ref[coords + (slice(None), slice(0, SLABS * ROWS))] = labown_ref[...]
        ag_start(0, 0)
        w_copy = remote(w_hbm, w_ref.at[core], w_send, w_recv, partner)
        w_copy.start()
        lab_start(0)
        ag_wait(0, 0)
        ag_start(0, 1)
        ag_start(1, 0)
        lab_wait(0)
        lab_start(1)
        ag_wait(0, 1)
        lab_wait(1)
        lab_start(2)
        ag_start(0, 2)
        ag_wait(1, 0)
        ag_start(1, 1)
        lab_wait(2)

    lane16 = lax.broadcasted_iota(jnp.int32, (ROWS, LANES), 1)
    row16 = lax.broadcasted_iota(jnp.int32, (ROWS, LANES), 0)
    first_col = chip * (2 * HALF)

    def spread(k, carry):
        kz, ky, kx = lax.div(k, 16), lax.rem(lax.div(k, 4), 4), lax.rem(k, 4)
        row = jnp.broadcast_to(labrow_ref[kz, ky, kx], (ROWS, LANES)).astype(F32)
        for s in range(SLABS):
            col = jnp.sum(jnp.where(lane16 == row16 + ROWS * s, row, 0.0), axis=1, keepdims=True)
            lab_ref[s, k] = jnp.broadcast_to(col, (ROWS, LANES)).astype(jnp.int32) - first_col - lane16
        return carry

    with jax.named_scope("spread"):
        lax.fori_loop(0, 64, spread, 0, unroll=4)

    def p_copy(n, slot):
        return pltpu.make_async_copy(buf_ref.at[slot, pl.ds(0, 1024)], p_hbm.at[n], p_sem.at[slot])

    def plane(k):
        return lax.rem(coords[0] + k + 1, SIDE)

    def g_load(t):
        slot = lax.rem(t, 2)
        n = lax.div(t, SIDE) * SIDE + plane(lax.rem(t, SIDE))
        return pltpu.make_async_copy(p_hbm.at[n], buf_ref.at[slot, pl.ds(0, 1024)], g_sem.at[slot])

    def st_copy(s, axis, d):
        view = st_ref.at[s, axis, coords[axis]]
        return remote(view, view, st_send.at[s, axis], st_recv.at[s, axis], rank(axis, d))

    def st_all(s, axis):
        view = st_ref.at[s, axis, pl.ds(0, 3)]
        return remote(view, view, st_send.at[s, axis], st_recv.at[s, axis], partner)

    def st_start(s, axis):
        for d in (2, 1, 3):
            st_copy(s, axis, d).start()

    def st_merge(s, axis):
        with jax.named_scope("st_wait"):
            st_all(s, axis).wait_recv()
        top = st_ref[s, axis, 0, 0]
        for i in range(1, SIDE):
            top = jnp.maximum(top, st_ref[s, axis, i, 0])
        total = jnp.zeros_like(top)
        target = jnp.zeros_like(top)
        for i in range(SIDE):
            total += st_ref[s, axis, i, 1] * jnp.exp(st_ref[s, axis, i, 0] - top)
            target += st_ref[s, axis, i, 2]
        if axis < 2:
            here = coords[axis + 1]
            st_ref[s, axis + 1, here, 0] = top
            st_ref[s, axis + 1, here, 1] = total
            st_ref[s, axis + 1, here, 2] = target
            st_start(s, axis + 1)
        else:
            fin_ref[s, 0] = top
            fin_ref[s, 1] = INV / total
            fin_ref[s, 2] = top + jnp.log(total) - target

    def logits_block(s, b):
        n = s * SIDE + b
        slot = lax.rem(n, 2)

        @pl.when(n >= 2)
        def _():
            p_copy(n - 2, slot).wait()

        with jax.named_scope("z_dot"):
            xb = x_ref[s, b].reshape(BLOCK, HID)
            for q in range(4):
                buf_ref[slot, pl.ds(q * BLOCK, BLOCK), :] = jnp.dot(
                    xb, w_ref[q // 2, :, (q % 2) * 1024:(q % 2 + 1) * 1024], preferred_element_type=F32)

        @pl.when(n == 0)
        def _():
            ag_wait(1, 1)
            ag_start(1, 2)

        @pl.when(n == 2 * SIDE - 1)
        def _():
            p_copy(2 * SIDE - 2, 0).wait()
            g_load(0).start()

        def rows(i, carry):
            r0 = pl.multiple_of(i * 8, 8)
            lab = lab_ref[s, b * 16 + lax.div(i, 2), pl.ds(pl.multiple_of(lax.rem(i, 2) * 8, 8), 8), :]
            z = [buf_ref[slot, pl.ds(pl.multiple_of(q * BLOCK + r0, 8), 8), l * LANES:(l + 1) * LANES]
                 for q in range(4) for l in range(8)]
            tops = z
            while len(tops) > 1:
                tops = [jnp.maximum(tops[k], tops[k + 1]) for k in range(0, len(tops), 2)]
            top = tops[0]
            sums = [jnp.zeros((8, LANES), F32) for _ in range(2)]
            tgt = [jnp.zeros((8, LANES), F32) for _ in range(2)]
            for k in range(32):
                p = jnp.exp(z[k] - top)
                q, l = k // 8, k % 8
                buf_ref[slot, pl.ds(pl.multiple_of(q * BLOCK + r0, 8), 8), l * LANES:(l + 1) * LANES] = p
                sums[k % 2] += p
                tgt[k % 2] = jnp.where(lab == k * LANES, z[k], tgt[k % 2])
            m_ref[s, pl.ds(pl.multiple_of(b * BLOCK + r0, 8), 8), :] = top
            s_ref[pl.ds(r0, 8), :] = sums[0] + sums[1]
            t_ref[pl.ds(r0, 8), :] = tgt[0] + tgt[1]
            return carry

        with jax.named_scope("z_rows"):
            lax.fori_loop(0, BLOCK // 8, rows, 0, unroll=2)
        p_copy(n, slot).start()
        with jax.named_scope("z_stat"):
            for i in range(2):
                m_t = m_ref[s, pl.ds(pl.multiple_of(b * BLOCK + i * LANES, LANES), LANES), :].T
                s_t = s_ref[i * LANES:(i + 1) * LANES, :].T
                t_t = t_ref[i * LANES:(i + 1) * LANES, :].T
                top = jnp.max(m_t, axis=0, keepdims=True)
                at = pl.ds(b * 2 + i, 1)
                srow_ref[0, at, :] = top
                srow_ref[1, at, :] = jnp.sum(s_t * jnp.exp(m_t - top), axis=0, keepdims=True)
                srow_ref[2, at, :] = jnp.sum(t_t, axis=0, keepdims=True)

    def st_begin(s):
        for k in range(3):
            st_ref[s, 0, coords[0], k] = srow_ref[k]
        st_start(s, 0)

    def rs_copy(s, phase, c, d):
        order = ORDERS[c]
        idx = [slice(None)] * 3
        for a in order[:phase]:
            idx[a] = coords[a]
        idx[order[phase]] = ring(order[phase], d)
        land = (r1_ref, r2_ref, r3_ref)[phase]
        return remote(dx_ref.at[(s,) + tuple(idx) + (slice(None), cols(c))], land.at[s, c, d - 1],
                      rs_send.at[s, phase], rs_recv.at[s, phase], rank(order[phase], d))

    def rs_plane(s, k, c, d):
        axis = ORDERS[c][0]
        b = plane(k)
        idx = [b, slice(None), slice(None)]
        if axis:
            idx[axis] = ring(axis, d)
        return remote(dx_ref.at[(s,) + tuple(idx) + (slice(None), cols(c))], r1_ref.at[s, c, d - 1, b],
                      rs_send.at[s, 0], rs_recv.at[s, 0], rank(axis, d))

    def rs_line(s, k):
        b = plane(k)
        return remote(dx_ref.at[s, b, :, :, :, cols(2)], r1_ref.at[s, 2, k],
                      rs_send.at[s, 0], rs_recv.at[s, 0], rank(0, k + 1))

    def rs_first(s, k):
        for d in (2, 1, 3):
            for c in range(2):
                rs_plane(s, k, c, d).start()

        @pl.when(k < SIDE - 1)
        def _():
            rs_line(s, k).start()

    def rs_all(s, phase):
        view = (r1_ref.at[s], r2_ref.at[s], r3_ref.at[s])[phase]
        return remote(view, view, rs_send.at[s, phase], rs_recv.at[s, phase], partner)

    def rs_start(s, phase):
        for d in (2, 1, 3):
            for c in range(3):
                rs_copy(s, phase, c, d).start()

    def rs_add(s, phase):
        with jax.named_scope("rs_wait"):
            rs_all(s, phase).wait_recv()
        for c in range(3):
            order = ORDERS[c]
            sl = slice(c * COLOUR, (c + 1) * COLOUR)
            idx = [None] * 3
            for a in order[:phase + 1]:
                idx[a] = coords[a]
            free = [a for a in range(3) if idx[a] is None]
            if phase == 0:
                def add(i, carry):
                    for j in range(SIDE):
                        at = list(idx)
                        at[free[0]], at[free[1]] = i, j
                        at = (s,) + tuple(at)
                        dx_ref[at + (slice(None), sl)] = (
                            (dx_ref[at + (slice(None), sl)] + r1_ref[s, c, 0, i, j])
                            + (r1_ref[s, c, 1, i, j] + r1_ref[s, c, 2, i, j]))
                    return carry
                lax.fori_loop(0, SIDE, add, 0)
            elif phase == 1:
                def add(i, carry):
                    at = list(idx)
                    at[free[0]] = i
                    at = (s,) + tuple(at)
                    dx_ref[at + (slice(None), sl)] = (
                        (dx_ref[at + (slice(None), sl)] + r2_ref[s, c, 0, i])
                        + (r2_ref[s, c, 1, i] + r2_ref[s, c, 2, i]))
                    return carry
                lax.fori_loop(0, SIDE, add, 0)
            else:
                total = ((dx_ref[(s,) + tuple(idx) + (slice(None), sl)] + r3_ref[s, c, 0])
                         + (r3_ref[s, c, 1] + r3_ref[s, c, 2]))
                dhid_ref[s * ROWS:(s + 1) * ROWS, sl] = total.astype(BF16)
        if phase < 2:
            rs_start(s, phase + 1)

    def grad_block(s, k):
        b = plane(k)
        n = s * SIDE + b
        t = s * SIDE + k
        slot = lax.rem(t, 2)

        with jax.named_scope("g_scale"):
            for i in range(2):
                at = pl.ds(b * 2 + i, 1)
                top = jnp.broadcast_to(fin_ref[s, 0, at, :], (LANES, LANES)).T
                inv = jnp.broadcast_to(fin_ref[s, 1, at, :], (LANES, LANES)).T
                m = m_ref[s, pl.ds(pl.multiple_of(b * BLOCK + i * LANES, LANES), LANES), :]
                scale_ref[i * LANES:(i + 1) * LANES, :] = jnp.exp(m - top) * inv
        g_load(t).wait()

        def rows(i, carry):
            r0 = pl.multiple_of(i * ROWS, ROWS)
            lab = lab_ref[s, b * 16 + i]
            scale = scale_ref[pl.ds(r0, ROWS), :]
            out_row = pl.multiple_of(n * BLOCK + r0, ROWS)
            for k in range(32):
                q, l = k // 8, k % 8
                p = buf_ref[slot, pl.ds(pl.multiple_of(q * BLOCK + r0, 8), ROWS), l * LANES:(l + 1) * LANES]
                g = p * scale - jnp.where(lab == k * LANES, INV, 0.0)
                g_ref[k // 16, pl.ds(out_row, ROWS), (k % 16) * LANES:(k % 16 + 1) * LANES] = g.astype(BF16)
            return carry

        with jax.named_scope("g_rows"):
            lax.fori_loop(0, BLOCK // ROWS, rows, 0, unroll=2)

        @pl.when(t == 0)
        def _():
            p_copy(2 * SIDE - 1, 1).wait()
            st_merge(1, 0)

        @pl.when(t < 2 * SIDE - 1)
        def _():
            g_load(t + 1).start()

        at = pl.ds(pl.multiple_of(n * BLOCK, BLOCK), BLOCK)
        nt = (((1,), (1,)), ((), ()))
        with jax.named_scope("dx_dot"):
            dx = (lax.dot_general(g_ref[0, at, :], w_ref[0], nt, preferred_element_type=F32)
                  + lax.dot_general(g_ref[1, at, :], w_ref[1], nt, preferred_element_type=F32))
            dx_ref[s, b] = dx.reshape(SIDE, SIDE, ROWS, HID)
        pl.when(t == 0)(functools.partial(st_merge, 1, 1))
        rs_first(s, k)

    with jax.named_scope("first_wait"):
        w_own.wait()
        w_copy.wait_recv()
        ag_wait(0, 2)

    def logits_first(b, carry):
        logits_block(0, b)
        return carry

    lax.fori_loop(0, SIDE, logits_first, 0)
    st_begin(0)
    with jax.named_scope("second_wait"):
        ag_wait(1, 2)

    def logits_second(b, carry):
        logits_block(1, b)
        for axis in range(3):
            pl.when(b == axis)(functools.partial(st_merge, 0, axis))
        return carry

    lax.fori_loop(0, SIDE, logits_second, 0)
    st_begin(1)

    def grad_first(b, carry):
        grad_block(0, b)
        pl.when(b == 2)(functools.partial(st_merge, 1, 2))
        return carry

    lax.fori_loop(0, SIDE, grad_first, 0)

    lossx_ref[core] = fin_ref[0, 2] + fin_ref[1, 2]
    ls_copy = remote(lossx_ref.at[core], lossx_ref.at[core], ls_send, ls_recv, partner)
    ls_copy.start()

    def grad_second(b, carry):
        grad_block(1, b)
        pl.when(b == 2)(functools.partial(rs_add, 0, 0))
        return carry

    lax.fori_loop(0, SIDE, grad_second, 0)
    ls_copy.wait_recv()
    loss_ref[0] = jnp.sum(lossx_ref[0] + lossx_ref[1]) * INV

    def flip(k, carry):
        kz, ky = lax.div(lax.rem(k, 8), 2), lax.rem(k, 2) * 2
        xs = x_ref[lax.div(k, 8), kz, pl.ds(ky, 2)].reshape(LANES, HID)
        w_ref[1, :, pl.ds(pl.multiple_of(k * LANES, LANES), LANES)] = xs.T
        return carry

    with jax.named_scope("flip"):
        lax.fori_loop(0, 2 * 1024 // LANES, flip, 0)

    def half(slot):
        return pl.ds(pl.multiple_of(slot * 512, 512), 512)

    def head_copy(j):
        slot = lax.rem(j, 2)
        return remote(buf_ref.at[0, :, half(slot)], hrecv_hbm.at[j], hd_send.at[slot], hd_recv.at[j], partner)

    def head_load(j):
        return pltpu.make_async_copy(hrecv_hbm.at[j], buf_ref.at[1, :, pl.ds(512, 512)], h_sem)

    def head_dot(h, j):
        with jax.named_scope("h_dot"):
            return jnp.dot(w_ref[1], g_ref[h, :, half(j)], preferred_element_type=F32)

    def out_copy(j):
        return pltpu.make_async_copy(w_ref.at[0, :, half(j)], dhead_hbm.at[:, half(j)], out_sem.at[j])

    def theirs(j):
        @pl.when(jnp.int32(j) >= 2)
        def _():
            head_copy(j - 2).wait_send()

        buf_ref[0, :, half(lax.rem(j, 2))] = head_dot(1 - core, j)
        head_copy(j).start()

    def ours(j):
        with jax.named_scope("h_wait"):
            head_copy(j).wait_recv()
        head_load(j).start()
        buf_ref[1, :, pl.ds(0, 512)] = head_dot(core, j)
        with jax.named_scope("h_load"):
            head_load(j).wait()

        def add(i, carry):
            r = pl.ds(pl.multiple_of(i * 16, 16), 16)
            w_ref[0, r, half(j)] = (buf_ref[1, r, pl.ds(0, 512)] + buf_ref[1, r, pl.ds(512, 512)]).astype(BF16)
            return carry

        with jax.named_scope("h_add"):
            lax.fori_loop(0, HID // 16, add, 0, unroll=4)
        out_copy(j).start()

    def pair(r, carry):
        theirs(r + 1)
        pl.when(r == 1)(functools.partial(rs_add, 0, 1))
        pl.when(r == 2)(functools.partial(rs_add, 1, 1))
        ours(r)
        pl.when(r == 0)(functools.partial(rs_add, 1, 0))
        pl.when(r == 2)(functools.partial(rs_add, 0, 2))
        return carry

    theirs(0)
    lax.fori_loop(0, 3, pair, 0)
    ours(3)
    rs_add(1, 2)
    head_copy(2).wait_send()
    head_copy(3).wait_send()

    with jax.named_scope("tail"):
        for j in range(4):
            out_copy(j).wait()
        w_copy.wait_send()
        ls_copy.wait_send()
        for phase in range(3):
            lab_all(phase).wait_send()
            for s in range(SLABS):
                st_all(s, phase).wait_send()
                ag_all(s, phase).wait_send()
                rs_all(s, phase).wait_send()


PIECES = 8


def hand_out(loss_in, dhid_in, dhead_in, loss_out, dhid_out, dhead_out, dhid_v, dhead_v, in_sem, out_sem):
    ways = [(dhid_in, dhid_v, dhid_out)]
    for i in range(PIECES):
        at = pl.ds(i * (HID // PIECES), HID // PIECES)
        ways.append((dhead_in.at[at], dhead_v.at[at], dhead_out.at[at]))
    ins = [pltpu.make_async_copy(a, v, in_sem.at[i]) for i, (a, v, _) in enumerate(ways)]
    outs = [pltpu.make_async_copy(v, o, out_sem.at[i]) for i, (_, v, o) in enumerate(ways)]
    for copy in ins:
        copy.start()
    loss_out[0] = loss_in[0]
    for here, there in zip(ins, outs):
        here.wait()
        there.start()
    for copy in outs:
        copy.wait()


def solution(mesh):
    any_space = pl.BlockSpec(memory_space=pl.ANY)
    vmem = pl.BlockSpec(memory_space=pltpu.VMEM)
    smem = pl.BlockSpec(memory_space=pltpu.SMEM)
    dma = pltpu.SemaphoreType.DMA

    def local_step(hid_loc, w_loc, lab_loc):
        labels = lab_loc.reshape(1, -1)
        flops = 3 * 2 * TOKENS * HID * HALF
        loss, d_hidden, d_head, _, _ = pl.pallas_call(
            body,
            out_shape=(
                jax.ShapeDtypeStruct((1,), F32),
                jax.ShapeDtypeStruct((SLABS * ROWS, HID), BF16),
                jax.ShapeDtypeStruct((HID, HALF), BF16),
                jax.ShapeDtypeStruct((8, 1024, 1024), F32),
                jax.ShapeDtypeStruct((4, HID, 512), F32),
            ),
            in_specs=[any_space, any_space, any_space],
            out_specs=(smem, vmem, any_space, any_space, any_space),
            scratch_shapes=[
                pltpu.VMEM((SLABS, SIDE, SIDE, SIDE, ROWS, HID), BF16),
                pltpu.VMEM((2, HID, HALF), BF16),
                pltpu.VMEM((2, 2048, HALF), BF16),
                pltpu.VMEM((SLABS, SIDE, SIDE, SIDE, ROWS, HID), F32),
                pltpu.VMEM((2, HID, 1024), F32),
                pltpu.VMEM((SLABS, 3, 3, SIDE, SIDE, ROWS, COLOUR), F32),
                pltpu.VMEM((SLABS, 3, 3, SIDE, ROWS, COLOUR), F32),
                pltpu.VMEM((SLABS, 3, 3, ROWS, COLOUR), F32),
                pltpu.VMEM((1, SLABS * ROWS), jnp.int32),
                pltpu.VMEM((SIDE, SIDE, SIDE, 1, LANES), jnp.int32),
                pltpu.VMEM((SLABS, 64, ROWS, LANES), jnp.int32),
                pltpu.VMEM((SLABS, 1024, LANES), F32),
                pltpu.VMEM((BLOCK, LANES), F32),
                pltpu.VMEM((BLOCK, LANES), F32),
                pltpu.VMEM((BLOCK, LANES), F32),
                pltpu.VMEM((3, 8, LANES), F32),
                pltpu.VMEM((SLABS, 3, SIDE, 3, 8, LANES), F32),
                pltpu.VMEM((SLABS, 3, 8, LANES), F32),
                pltpu.VMEM((2, 8, LANES), F32),
                dma((SLABS, 3)), dma((SLABS, 3)),
                dma((3,)), dma((3,)),
                dma, dma,
                dma((SLABS, 3)), dma((SLABS, 3)),
                dma((SLABS, 3)), dma((SLABS, 3)),
                dma((2,)), dma((4,)),
                dma, dma,
                dma((4,)), dma((2,)), dma((2,)), dma, dma((4,)),
            ],
            compiler_params=pltpu.CompilerParams(
                collective_id=0, has_side_effects=True, vmem_limit_bytes=67043328),
            cost_estimate=pl.CostEstimate(flops=flops, bytes_accessed=100_000_000, transcendentals=TOKENS * HALF),
        )(hid_loc, w_loc, labels)
        return pl.pallas_call(
            hand_out,
            out_shape=(
                jax.ShapeDtypeStruct((1,), F32),
                jax.ShapeDtypeStruct((SLABS * ROWS, HID), BF16),
                jax.ShapeDtypeStruct((HID, HALF), BF16),
            ),
            in_specs=[smem, any_space, any_space],
            out_specs=(smem, any_space, any_space),
            scratch_shapes=[
                pltpu.VMEM((SLABS * ROWS, HID), BF16),
                pltpu.VMEM((HID, HALF), BF16),
                dma((PIECES + 1,)), dma((PIECES + 1,)),
            ],
        )(loss, d_hidden, d_head)

    return jax.shard_map(
        local_step,
        mesh=mesh,
        in_specs=(P(("dp", "tp"), None), P(None, "tp"), P(("dp", "tp"))),
        out_specs=(P("dp"), P(("dp", "tp"), None), P("dp", "tp")),
        check_vma=False,
    )
```

```python
import functools

import jax
import jax.numpy as jnp
from jax import lax
from jax.experimental import pallas as pl
from jax.experimental.pallas import tpu as pltpu
from jax.sharding import PartitionSpec as P

MESH = pl.DeviceIdType.MESH
F32 = jnp.float32
BF16 = jnp.bfloat16

SIDE = 4
STRIDES = (32, 8, 2)
ORDERS = ((2, 1, 0), (1, 0, 2), (0, 2, 1))
SLABS = 2
ROWS = 16
BLOCK = 256
HID = 1152
COLOUR = HID // 3
HEAD_ROWS = 384
WIDE = 1024
HEAD = 512
SUB = 8
ALL = slice(None)
FAR = (2, 1, 3)
NEXT = (1, 2, 3)
THREE = pl.ds(0, 3)
FULL = pl.ds(0, WIDE)
HALF = 2048
TOKENS = 4096
INV = 1.0 / TOKENS
LANES = 128


def body(x_hbm, w_hbm, lab_hbm,
         loss_ref, dhid_ref, dhead_hbm, p_hbm, hrecv_hbm,
         x_ref, w_ref, ga_ref, gb_ref, dx_ref, bufa_ref, bufb_ref, r1_ref, r2_ref, r3_ref,
         labown_ref, labrow_ref, lab_ref, m_ref, mt_ref, s_ref, t_ref, srow_ref, st_ref, fin_ref, lossx_ref,
         ag_send, ag_recv, a3_send, a3_recv, lab_send, lab_recv, w_send, w_recv, st_send, st_recv, rs_send, rs_recv,
         hd_send, hd_recv, ls_send, ls_recv, in_sem, p_sem, g_sem, h_sem, out_sem):
    me = lax.axis_index("tp")
    core = lax.rem(me, 2)
    chip = lax.div(me, 2)
    coords = (lax.div(chip, ROWS), lax.rem(lax.div(chip, 4), 4), lax.rem(chip, 4))
    partner = me + 1 - 2 * core

    def ring(axis, d):
        return lax.rem(coords[axis] + d, SIDE)

    def rank(axis, d):
        return me + (ring(axis, d) - coords[axis]) * STRIDES[axis]

    def remote(src, dst, send, recv, target):
        return pltpu.make_async_remote_copy(src_ref=src, dst_ref=dst, send_sem=send, recv_sem=recv,
                                            device_id={"tp": target}, device_id_type=MESH)

    def cols(c):
        return pl.ds(COLOUR * c, COLOUR)

    own = []
    for s in range(SLABS):
        own.append(pltpu.make_async_copy(x_hbm.at[pl.ds(ROWS * s, ROWS)],
                                         x_ref.at[(s,) + coords], in_sem.at[s]))
    own.append(pltpu.make_async_copy(lab_hbm, labown_ref, in_sem.at[2]))
    w_own = pltpu.make_async_copy(w_hbm, w_ref.at[core], in_sem.at[3])
    for copy in own:
        copy.start()
    w_own.start()

    with jax.named_scope("meet"):
        barrier = pltpu.get_barrier_semaphore()
        peers = [partner] + [rank(a, d) for a in range(3) for d in NEXT]
        for peer in peers:
            pl.semaphore_signal(barrier, inc=1, device_id={"tp": peer}, device_id_type=MESH)
        pl.semaphore_wait(barrier, len(peers))

    def ag_copy(s, phase, c, d):
        order = ORDERS[c]
        idx = list(coords)
        for a in order[:phase]:
            idx[a] = ALL
        view = x_ref.at[(s,) + tuple(idx) + (ALL, cols(c))]
        return remote(view, view, ag_send.at[s, phase], ag_recv.at[s, phase],
                      rank(order[phase], d))

    def ag_start(s, phase):
        for d in FAR:
            for c in range(3):
                ag_copy(s, phase, c, d).start()

    def ag_all(s, phase):
        view = (x_ref.at[s, 0, 0, THREE], x_ref.at[s, 0, THREE], x_ref.at[s, THREE])[phase]
        return remote(view, view, ag_send.at[s, phase], ag_recv.at[s, phase], partner)

    def ag_wait(s, phase):
        ag_all(s, phase).wait_recv()

    def near(k):
        return lax.rem(coords[0] + k, SIDE)

    def ag_plane(k, c, d):
        axis = ORDERS[c][2]
        idx = [near(k), ALL, ALL]
        idx[axis] = coords[axis]
        view = x_ref.at[(0,) + tuple(idx) + (ALL, cols(c))]
        return remote(view, view, a3_send.at[0], a3_recv.at[0, k], rank(axis, d))

    def ag_line(k):
        view = x_ref.at[0, coords[0], :, :, :, cols(0)]
        return remote(view, view, a3_send.at[1], a3_recv.at[1, k], rank(0, SIDE - k))

    def ag_near(k):
        for d in FAR:
            for c in (1, 2):
                ag_plane(k, c, d).start()
        if k:
            ag_line(k).start()

    def ag_near_wait(k):
        view = x_ref.at[0, pl.ds(0, 2), 0]
        remote(view, view, a3_send.at[0], a3_recv.at[0, k], partner).wait_recv()

    def ag_line_wait(k):
        view = x_ref.at[0, 0, :, :, :, cols(0)]
        remote(view, view, a3_send.at[1], a3_recv.at[1, k], partner).wait_recv()

    def ag_near_sent():
        view = x_ref.at[0, pl.ds(0, 2)]
        remote(view, view, a3_send.at[0], a3_recv.at[0, 0], partner).wait_send()
        view = x_ref.at[0, THREE, :, :, :, cols(0)]
        remote(view, view, a3_send.at[1], a3_recv.at[1, 0], partner).wait_send()

    def lab_copy(phase, d):
        order = ORDERS[0]
        idx = list(coords)
        for a in order[:phase]:
            idx[a] = ALL
        view = labrow_ref.at[tuple(idx)]
        return remote(view, view, lab_send.at[phase], lab_recv.at[phase], rank(order[phase], d))

    def lab_start(phase):
        for d in NEXT:
            lab_copy(phase, d).start()

    def lab_all(phase):
        view = (labrow_ref.at[0, 0, THREE], labrow_ref.at[0, THREE], labrow_ref.at[THREE])[phase]
        return remote(view, view, lab_send.at[phase], lab_recv.at[phase], partner)

    def lab_wait(phase):
        lab_all(phase).wait_recv()

    with jax.named_scope("ag"):
        for copy in own:
            copy.wait()
        labrow_ref[coords + (ALL, slice(0, SLABS * ROWS))] = labown_ref[...]
        ag_start(0, 0)
        w_copy = remote(w_hbm, w_ref.at[core], w_send, w_recv, partner)
        w_copy.start()
        lab_start(0)
        ag_wait(0, 0)
        ag_start(0, 1)
        ag_start(1, 0)
        lab_wait(0)
        lab_start(1)
        ag_wait(0, 1)
        lab_wait(1)
        lab_start(2)
        ag_near(0)
        ag_near(1)
        ag_wait(1, 0)
        ag_start(1, 1)
        ag_near(2)
        ag_near(3)
        lab_wait(2)

    lane16 = lax.broadcasted_iota(jnp.int32, (ROWS, LANES), 1)
    row16 = lax.broadcasted_iota(jnp.int32, (ROWS, LANES), 0)
    first_col = chip * (2 * HALF)

    def spread(k, carry):
        kz, ky, kx = lax.div(k, ROWS), lax.rem(lax.div(k, 4), 4), lax.rem(k, 4)
        row = jnp.broadcast_to(labrow_ref[kz, ky, kx], (ROWS, LANES)).astype(F32)
        for s in range(SLABS):
            col = jnp.sum(jnp.where(lane16 == row16 + ROWS * s, row, 0.0), axis=1, keepdims=True)
            lab_ref[s, k] = jnp.broadcast_to(col, (ROWS, LANES)).astype(jnp.int32) - first_col - lane16
        return carry

    with jax.named_scope("spread"):
        lax.fori_loop(0, 64, spread, 0, unroll=4)

    bufs = (bufa_ref, bufb_ref)

    def p_copy(n, slot, q, r, rows):
        at = pl.ds(pl.multiple_of(q * BLOCK + r, SUB), rows)
        return pltpu.make_async_copy(bufs[slot].at[at], p_hbm.at[n, at], p_sem.at[slot])

    def p_start(n, slot, r, rows):
        for q in range(4):
            p_copy(n, slot, q, r, rows).start()

    def p_wait(n, slot):
        at = FULL
        pltpu.make_async_copy(bufs[slot].at[at], p_hbm.at[n], p_sem.at[slot]).wait()

    def plane(k):
        return lax.rem(coords[0] + k + 1, SIDE)

    def place(t):
        return lax.div(t, SIDE), plane(lax.rem(t, SIDE))

    def g_load(t, slot):
        s, b = place(t)
        return pltpu.make_async_copy(p_hbm.at[s * SIDE + b], bufs[slot].at[FULL], g_sem.at[slot])

    def p_ahead():
        n = plane(0)

        def line(j, carry):
            q, y, x = lax.div(j, ROWS), lax.rem(lax.div(j, 4), 4), lax.rem(j, 4)
            pltpu.make_async_copy(p_hbm.at[n, pl.ds(pl.multiple_of(j * ROWS, ROWS), ROWS)],
                                  dx_ref.at[1, q, y, x, :, FULL], g_sem.at[2]).start()
            return carry

        lax.fori_loop(0, 64, line, 0)

    def p_there():
        at = FULL
        pltpu.make_async_copy(p_hbm.at[0], bufa_ref.at[at], g_sem.at[2]).wait()

    def st_copy(s, axis, d):
        view = st_ref.at[s, axis, coords[axis]]
        return remote(view, view, st_send.at[s, axis], st_recv.at[s, axis], rank(axis, d))

    def st_all(s, axis):
        view = st_ref.at[s, axis, THREE]
        return remote(view, view, st_send.at[s, axis], st_recv.at[s, axis], partner)

    def st_start(s, axis):
        for d in FAR:
            st_copy(s, axis, d).start()

    def st_merge(s, axis):
        with jax.named_scope("st_wait"):
            st_all(s, axis).wait_recv()
        top = st_ref[s, axis, 0, 0]
        for i in range(1, SIDE):
            top = jnp.maximum(top, st_ref[s, axis, i, 0])
        total = jnp.zeros_like(top)
        target = jnp.zeros_like(top)
        for i in range(SIDE):
            total += st_ref[s, axis, i, 1] * jnp.exp(st_ref[s, axis, i, 0] - top)
            target += st_ref[s, axis, i, 2]
        if axis < 2:
            here = coords[axis + 1]
            st_ref[s, axis + 1, here, 0] = top
            st_ref[s, axis + 1, here, 1] = total
            st_ref[s, axis + 1, here, 2] = target
            st_start(s, axis + 1)
        else:
            fin_ref[s, 0] = top
            fin_ref[s, 1] = INV / total
            fin_ref[s, 2] = top + jnp.log(total) - target

    def z_group(n, slot, i):
        buf = bufs[slot]
        s, b = lax.div(n, SIDE), lax.rem(n, SIDE)
        at = [pl.ds(pl.multiple_of(q * BLOCK + i * SUB, SUB), SUB) for q in range(4)]
        part, row = pl.ds(pl.multiple_of(lax.rem(i, 2) * SUB, SUB), SUB), lax.div(i, 2)
        here = pl.ds(pl.multiple_of(i * SUB, SUB), SUB)
        lab = lab_ref[s, b * ROWS + row, part, :]
        z = [buf[at[q], l * LANES:(l + 1) * LANES] for q in range(4) for l in range(SUB)]
        tops = z
        while len(tops) > 1:
            tops = [jnp.maximum(tops[k], tops[k + 1]) for k in range(0, len(tops), 2)]
        top = tops[0]
        sums = [jnp.zeros((SUB, LANES), F32) for _ in range(2)]
        tgt = [jnp.zeros((SUB, LANES), F32) for _ in range(2)]
        for k in range(32):
            p = jnp.exp(z[k] - top)
            buf[at[k // SUB], k % SUB * LANES:(k % SUB + 1) * LANES] = p
            sums[k % 2] += p
            tgt[k % 2] = jnp.where(lab == k * LANES, z[k], tgt[k % 2])
        mt_ref[here, :] = top
        s_ref[here, :] = sums[0] + sums[1]
        t_ref[here, :] = tgt[0] + tgt[1]

    def z_stat(n):
        s, b = lax.div(n, SIDE), lax.rem(n, SIDE)
        for i in range(2):
            m = mt_ref[i * LANES:(i + 1) * LANES, :]
            m_ref[s, pl.ds(pl.multiple_of(b * BLOCK + i * LANES, LANES), LANES), :] = m
            m_t = m.T
            s_t = s_ref[i * LANES:(i + 1) * LANES, :].T
            t_t = t_ref[i * LANES:(i + 1) * LANES, :].T
            top = jnp.max(m_t, axis=0, keepdims=True)
            at = pl.ds(b * 2 + i, 1)
            srow_ref[0, at, :] = top
            srow_ref[1, at, :] = jnp.sum(s_t * jnp.exp(m_t - top), axis=0, keepdims=True)
            srow_ref[2, at, :] = jnp.sum(t_t, axis=0, keepdims=True)

    def z_step(t, slot):
        s, k = lax.div(t, SIDE), lax.rem(t, SIDE)
        b = near(k)
        n = s * SIDE + b

        @pl.when(t >= 2)
        def _():
            p_wait(n, slot)

        with jax.named_scope("z_dot"):
            xb = x_ref[s, b].reshape(BLOCK, HID)
            for q in range(4):
                bufs[slot][pl.ds(q * BLOCK, BLOCK), :] = jnp.dot(
                    xb, w_ref[q // 2, :, q % 2 * WIDE:(q % 2 + 1) * WIDE], preferred_element_type=F32)
        if slot:
            @pl.when(t == 2 * SIDE - 1)
            def _():
                p_wait(n, 0)
                g_load(1, 0).start()

        def rows(i, carry):
            z_group(n, slot, i)
            return carry

        with jax.named_scope("z_rows"):
            lax.fori_loop(0, 32, rows, 0, unroll=4)
        p_start(n, slot, 0, BLOCK)
        with jax.named_scope("z_stat"):
            z_stat(n)

    def st_begin(s):
        for k in range(3):
            st_ref[s, 0, coords[0], k] = srow_ref[k]
        st_start(s, 0)

    def rs_copy(s, phase, c, d):
        order = ORDERS[c]
        idx = [ALL] * 3
        for a in order[:phase]:
            idx[a] = coords[a]
        idx[order[phase]] = ring(order[phase], d)
        land = (r1_ref, r2_ref, r3_ref)[phase]
        return remote(dx_ref.at[(s,) + tuple(idx) + (ALL, cols(c))], land.at[s, c, d - 1],
                      rs_send.at[s, phase], rs_recv.at[s, phase], rank(order[phase], d))

    def rs_plane(s, k, c, d):
        axis = ORDERS[c][0]
        b = plane(k)
        idx = [b, ALL, ALL]
        if axis:
            idx[axis] = ring(axis, d)
        return remote(dx_ref.at[(s,) + tuple(idx) + (ALL, cols(c))], r1_ref.at[s, c, d - 1, b],
                      rs_send.at[s, 0], rs_recv.at[s, 0], rank(axis, d))

    def rs_line(s, k):
        b = plane(k)
        return remote(dx_ref.at[s, b, :, :, :, cols(2)], r1_ref.at[s, 2, k],
                      rs_send.at[s, 0], rs_recv.at[s, 0], rank(0, k + 1))

    def rs_first(t):
        s, k = lax.div(t, SIDE), lax.rem(t, SIDE)
        for d in FAR:
            for c in range(2):
                rs_plane(s, k, c, d).start()

        @pl.when(k < SIDE - 1)
        def _():
            rs_line(s, k).start()

    def rs_all(s, phase):
        view = (r1_ref.at[s], r2_ref.at[s], r3_ref.at[s])[phase]
        return remote(view, view, rs_send.at[s, phase], rs_recv.at[s, phase], partner)

    def rs_start(s, phase):
        for d in FAR:
            for c in range(3):
                rs_copy(s, phase, c, d).start()

    def rs_add(s, phase):
        with jax.named_scope("rs_wait"):
            rs_all(s, phase).wait_recv()
        for c in range(3):
            order = ORDERS[c]
            sl = slice(c * COLOUR, (c + 1) * COLOUR)
            idx = [None] * 3
            for a in order[:phase + 1]:
                idx[a] = coords[a]
            free = [a for a in range(3) if idx[a] is None]
            if phase == 0:
                def add(i, carry):
                    for j in range(SIDE):
                        at = list(idx)
                        at[free[0]], at[free[1]] = i, j
                        at = (s,) + tuple(at)
                        dx_ref[at + (ALL, sl)] = (
                            (dx_ref[at + (ALL, sl)] + r1_ref[s, c, 0, i, j])
                            + (r1_ref[s, c, 1, i, j] + r1_ref[s, c, 2, i, j]))
                    return carry
                lax.fori_loop(0, SIDE, add, 0)
            elif phase == 1:
                def add(i, carry):
                    at = list(idx)
                    at[free[0]] = i
                    at = (s,) + tuple(at)
                    dx_ref[at + (ALL, sl)] = (
                        (dx_ref[at + (ALL, sl)] + r2_ref[s, c, 0, i])
                        + (r2_ref[s, c, 1, i] + r2_ref[s, c, 2, i]))
                    return carry
                lax.fori_loop(0, SIDE, add, 0)
            else:
                total = ((dx_ref[(s,) + tuple(idx) + (ALL, sl)] + r3_ref[s, c, 0])
                         + (r3_ref[s, c, 1] + r3_ref[s, c, 2]))
                dhid_ref[s * ROWS:(s + 1) * ROWS, sl] = total.astype(BF16)
        if phase < 2:
            rs_start(s, phase + 1)

    gs = (ga_ref, gb_ref)
    last = jnp.int32(2 * SIDE - 1)

    def g_scale(t):
        s, b = place(t)
        for i in range(2):
            at = pl.ds(b * 2 + i, 1)
            top = jnp.broadcast_to(fin_ref[s, 0, at, :], (LANES, LANES)).T
            inv = jnp.broadcast_to(fin_ref[s, 1, at, :], (LANES, LANES)).T
            m = m_ref[s, pl.ds(pl.multiple_of(b * BLOCK + i * LANES, LANES), LANES), :]
            s_ref[i * LANES:(i + 1) * LANES, :] = jnp.exp(m - top) * inv

    def g_group(t, slot, i, ahead=True):
        s, b = place(t)
        at = [pl.ds(pl.multiple_of(q * BLOCK + i * ROWS, ROWS), ROWS) for q in range(4)]
        here = pl.ds(pl.multiple_of(i * ROWS, ROWS), ROWS)
        lab = lab_ref[s, b * ROWS + i]
        scale = s_ref[here, :]
        out = pl.ds(pl.multiple_of(lax.div(t, 2) * BLOCK + i * ROWS, ROWS), ROWS)
        for k in range(32):
            lanes = slice(k % SUB * LANES, (k % SUB + 1) * LANES)
            if ahead:
                p = bufs[1 - slot][at[k // SUB], lanes]
            else:
                p = dx_ref[1, k // SUB, lax.div(i, 4), lax.rem(i, 4), :, lanes]
            g = p * scale - jnp.where(lab == k * LANES, INV, 0.0)
            gs[slot][k // ROWS, out, k % ROWS * LANES:(k % ROWS + 1) * LANES] = g.astype(BF16)

    nt = (((1,), (1,)), ((), ()))

    def dx_dot(t, slot, h):
        at = pl.ds(pl.multiple_of(lax.div(t, 2) * BLOCK, BLOCK), BLOCK)
        return lax.dot_general(gs[slot][h, at, :], w_ref[h], nt, preferred_element_type=F32)

    def dx_store(t, dx):
        s, b = place(t)
        dx_ref[s, b] = dx.reshape(SIDE, SIDE, ROWS, HID)

    def g_step(t, slot):
        with jax.named_scope("g_load"):
            g_load(t, 1 - slot).wait()

        @pl.when(t < 2 * SIDE - 1)
        def _():
            pl.when(t == 1)(functools.partial(p_wait, 0, 1))
            g_load(t + 1, slot).start()

        with jax.named_scope("g_step"):
            g_scale(t)
            for i in range(ROWS):
                g_group(t, slot, i)
            dx_store(t - 1, dx_dot(t - 1, 1 - slot, 0) + dx_dot(t - 1, 1 - slot, 1))

    with jax.named_scope("first_wait"):
        w_own.wait()
        w_copy.wait_recv()
        ag_near_wait(0)

    def z_pair(i, carry):
        t = 2 * i

        with jax.named_scope("z_wait"):
            @pl.when(i == 1)
            def _():
                ag_near_wait(2)
                ag_line_wait(2)

            pl.when(i == 2)(functools.partial(ag_wait, 1, 2))
        z_step(t, 0)
        with jax.named_scope("z_wait"):
            @pl.when(i == 0)
            def _():
                ag_wait(1, 1)
                ag_start(1, 2)
                ag_near_wait(1)
                ag_line_wait(1)

            @pl.when(i == 1)
            def _():
                ag_near_wait(3)
                ag_line_wait(3)

            pl.when(i == 2)(functools.partial(st_merge, 0, 0))
            pl.when(i == 3)(functools.partial(st_merge, 0, 2))
        z_step(t + 1, 1)

        @pl.when(i == 1)
        def _():
            st_begin(0)
            p_ahead()

        pl.when(i == 2)(functools.partial(st_merge, 0, 1))
        return carry

    lax.fori_loop(0, SIDE, z_pair, 0)
    st_begin(1)

    def g_first(i, carry):
        g_group(jnp.int32(0), 0, i, False)
        return carry

    with jax.named_scope("g_first"):
        g_scale(jnp.int32(0))
        p_there()
        lax.fori_loop(0, ROWS, g_first, 0, unroll=2)

    def g_pair(i, carry):
        t = 2 * i + 1
        g_step(t, 1)
        pl.when(i == 0)(functools.partial(st_merge, 1, 0))
        pl.when(i == 1)(functools.partial(st_merge, 1, 2))
        rs_first(t - 1)

        @pl.when(i < SIDE - 1)
        def _():
            g_step(t + 1, 0)
            pl.when(i == 0)(functools.partial(st_merge, 1, 1))
            rs_first(t)

        return carry

    lax.fori_loop(0, SIDE, g_pair, 0)
    with jax.named_scope("dx_last"):
        dx_store(last, dx_dot(last, 1, 0) + dx_dot(last, 1, 1))
    rs_first(last)
    rs_add(0, 0)

    lossx_ref[core] = fin_ref[0, 2] + fin_ref[1, 2]
    ls_copy = remote(lossx_ref.at[core], lossx_ref.at[core], ls_send, ls_recv, partner)
    ls_copy.start()

    ls_copy.wait_recv()
    loss_ref[0] = jnp.sum(lossx_ref[0] + lossx_ref[1]) * INV

    def flip(j, carry):
        t, part = lax.div(j, 2), lax.rem(j, 2)
        s, b = place(t)
        xs = x_ref[s, b, pl.ds(part * 2, 2)].reshape(LANES, HID)
        at = lax.rem(t, 2) * WIDE + lax.div(t, 2) * BLOCK + part * LANES
        w_ref[1, :, pl.ds(pl.multiple_of(at, LANES), LANES)] = xs.T
        return carry

    with jax.named_scope("flip"):
        lax.fori_loop(0, 2 * WIDE // LANES, flip, 0)

    def half(slot):
        return pl.ds(pl.multiple_of(slot * HEAD, HEAD), HEAD)

    def head_copy(j):
        slot = lax.rem(j, 2)
        return remote(bufa_ref.at[:, half(slot)], hrecv_hbm.at[j], hd_send.at[slot], hd_recv.at[j], partner)

    def head_load(j):
        return pltpu.make_async_copy(hrecv_hbm.at[j], bufb_ref.at[:, pl.ds(HEAD, HEAD)], h_sem)

    def head_dot(h, j, buf, at):
        with jax.named_scope("h_dot"):
            for r in range(0, HID, HEAD_ROWS):
                r = pl.ds(r, HEAD_ROWS)
                buf[r, at] = (jnp.dot(w_ref[1, r, :WIDE], ga_ref[h, :, half(j)], preferred_element_type=F32)
                              + jnp.dot(w_ref[1, r, WIDE:], gb_ref[h, :, half(j)], preferred_element_type=F32))

    def out_copy(j):
        return pltpu.make_async_copy(w_ref.at[0, :, half(j)], dhead_hbm.at[:, half(j)], out_sem.at[j])

    def theirs(j):
        @pl.when(jnp.int32(j) >= 2)
        def _():
            head_copy(j - 2).wait_send()

        head_dot(1 - core, j, bufa_ref, half(lax.rem(j, 2)))
        head_copy(j).start()

    def ours(j):
        head_dot(core, j, bufb_ref, pl.ds(0, HEAD))

    def fetch(j):
        with jax.named_scope("h_wait"):
            head_copy(j).wait_recv()
        head_load(j).start()

    def finish(j):
        with jax.named_scope("h_load"):
            head_load(j).wait()

        def add(i, carry):
            r = pl.ds(pl.multiple_of(i * ROWS, ROWS), ROWS)
            w_ref[0, r, half(j)] = (bufb_ref[r, pl.ds(0, HEAD)] + bufb_ref[r, pl.ds(HEAD, HEAD)]).astype(BF16)
            return carry

        with jax.named_scope("h_add"):
            lax.fori_loop(0, HID // ROWS, add, 0, unroll=SIDE)
        out_copy(j).start()

    def pair(r, carry):
        theirs(r + 1)

        @pl.when(r > 0)
        def _():
            finish(r - 1)

        pl.when(r == 1)(functools.partial(rs_add, 0, 1))
        ours(r)
        fetch(r)
        pl.when(r == 0)(functools.partial(rs_add, 1, 0))
        pl.when(r == 2)(functools.partial(rs_add, 1, 1))
        return carry

    theirs(0)
    lax.fori_loop(0, 3, pair, 0)
    rs_add(0, 2)
    finish(2)
    fetch(3)
    ours(3)
    finish(3)
    rs_add(1, 2)
    head_copy(2).wait_send()
    head_copy(3).wait_send()

    with jax.named_scope("tail"):
        for j in range(4):
            out_copy(j).wait()
        w_copy.wait_send()
        ls_copy.wait_send()
        ag_near_sent()
        for phase in range(3):
            lab_all(phase).wait_send()
            for s in range(SLABS):
                st_all(s, phase).wait_send()
                if s or phase < 2:
                    ag_all(s, phase).wait_send()
                rs_all(s, phase).wait_send()


PIECES = 8


def hand_out(loss_in, dhid_in, dhead_in, loss_out, dhid_out, dhead_out, dhid_v, dhead_v, in_sem, out_sem):
    ways = [(dhid_in, dhid_v, dhid_out)]
    for i in range(PIECES):
        at = pl.ds(i * (HID // PIECES), HID // PIECES)
        ways.append((dhead_in.at[at], dhead_v.at[at], dhead_out.at[at]))
    ins = [pltpu.make_async_copy(a, v, in_sem.at[i]) for i, (a, v, _) in enumerate(ways)]
    outs = [pltpu.make_async_copy(v, o, out_sem.at[i]) for i, (_, v, o) in enumerate(ways)]
    for copy in ins:
        copy.start()
    loss_out[0] = loss_in[0]
    for here, there in zip(ins, outs):
        here.wait()
        there.start()
    for copy in outs:
        copy.wait()


def solution(mesh):
    any_space = pl.BlockSpec(memory_space=pl.ANY)
    vmem = pl.BlockSpec(memory_space=pltpu.VMEM)
    smem = pl.BlockSpec(memory_space=pltpu.SMEM)
    dma = pltpu.SemaphoreType.DMA

    def local_step(hid_loc, w_loc, lab_loc):
        labels = lab_loc.reshape(1, -1)
        flops = 3 * 2 * TOKENS * HID * HALF
        loss, d_hidden, d_head, _, _ = pl.pallas_call(
            body,
            out_shape=(
                jax.ShapeDtypeStruct((1,), F32),
                jax.ShapeDtypeStruct((SLABS * ROWS, HID), BF16),
                jax.ShapeDtypeStruct((HID, HALF), BF16),
                jax.ShapeDtypeStruct((SUB, WIDE, WIDE), F32),
                jax.ShapeDtypeStruct((4, HID, HEAD), F32),
            ),
            in_specs=[any_space, any_space, any_space],
            out_specs=(smem, vmem, any_space, any_space, any_space),
            scratch_shapes=[
                pltpu.VMEM((SLABS, SIDE, SIDE, SIDE, ROWS, HID), BF16),
                pltpu.VMEM((2, HID, HALF), BF16),
                pltpu.VMEM((2, WIDE, HALF), BF16),
                pltpu.VMEM((2, WIDE, HALF), BF16),
                pltpu.VMEM((SLABS, SIDE, SIDE, SIDE, ROWS, HID), F32),
                pltpu.VMEM((HID, WIDE), F32),
                pltpu.VMEM((HID, WIDE), F32),
                pltpu.VMEM((SLABS, 3, 3, SIDE, SIDE, ROWS, COLOUR), F32),
                pltpu.VMEM((SLABS, 3, 3, SIDE, ROWS, COLOUR), F32),
                pltpu.VMEM((SLABS, 3, 3, ROWS, COLOUR), F32),
                pltpu.VMEM((1, SLABS * ROWS), jnp.int32),
                pltpu.VMEM((SIDE, SIDE, SIDE, 1, LANES), jnp.int32),
                pltpu.VMEM((SLABS, 64, ROWS, LANES), jnp.int32),
                pltpu.VMEM((SLABS, WIDE, LANES), F32),
                pltpu.VMEM((BLOCK, LANES), F32),
                pltpu.VMEM((BLOCK, LANES), F32),
                pltpu.VMEM((BLOCK, LANES), F32),
                pltpu.VMEM((3, SUB, LANES), F32),
                pltpu.VMEM((SLABS, 3, SIDE, 3, SUB, LANES), F32),
                pltpu.VMEM((SLABS, 3, SUB, LANES), F32),
                pltpu.VMEM((2, SUB, LANES), F32),
                dma((SLABS, 3)), dma((SLABS, 3)), dma((2,)), dma((2, SIDE)),
                dma((3,)), dma((3,)),
                dma, dma,
                dma((SLABS, 3)), dma((SLABS, 3)),
                dma((SLABS, 3)), dma((SLABS, 3)),
                dma((2,)), dma((4,)),
                dma, dma,
                dma((4,)), dma((2,)), dma((3,)), dma, dma((4,)),
            ],
            compiler_params=pltpu.CompilerParams(
                collective_id=0, has_side_effects=True, vmem_limit_bytes=67043328),
            cost_estimate=pl.CostEstimate(flops=flops, bytes_accessed=100_000_000, transcendentals=TOKENS * HALF),
        )(hid_loc, w_loc, labels)
        return pl.pallas_call(
            hand_out,
            out_shape=(
                jax.ShapeDtypeStruct((1,), F32),
                jax.ShapeDtypeStruct((SLABS * ROWS, HID), BF16),
                jax.ShapeDtypeStruct((HID, HALF), BF16),
            ),
            in_specs=[smem, any_space, any_space],
            out_specs=(smem, any_space, any_space),
            scratch_shapes=[
                pltpu.VMEM((SLABS * ROWS, HID), BF16),
                pltpu.VMEM((HID, HALF), BF16),
                dma((PIECES + 1,)), dma((PIECES + 1,)),
            ],
        )(loss, d_hidden, d_head)

    return jax.shard_map(
        local_step,
        mesh=mesh,
        in_specs=(P(("dp", "tp"), None), P(None, "tp"), P(("dp", "tp"))),
        out_specs=(P("dp"), P(("dp", "tp"), None), P("dp", "tp")),
        check_vma=False,
    )
```

```python
import functools

import jax
import jax.numpy as jnp
from jax import lax
from jax.experimental import pallas as pl
from jax.experimental.pallas import tpu as pltpu
from jax.sharding import PartitionSpec as P

MESH = pl.DeviceIdType.MESH
F32 = jnp.float32
BF16 = jnp.bfloat16

SIDE = 4
STRIDES = (32, 8, 2)
ORDERS = ((2, 1, 0), (1, 0, 2), (0, 2, 1))
SLABS = 2
ROWS = 16
BLOCK = 256
HID = 1152
COLOUR = HID // 3
HEAD_ROWS = 384
WIDE = 1024
HEAD = 512
SUB = 8
ALL = slice(None)
FAR = (2, 1, 3)
NEXT = (1, 2, 3)
THREE = pl.ds(0, 3)
FULL = pl.ds(0, WIDE)
HALF = 2048
TOKENS = 4096
INV = 1.0 / TOKENS
LANES = 128


def body(x_hbm, w_hbm, lab_hbm,
         loss_ref, dhid_ref, dhead_hbm, p_hbm, hrecv_hbm,
         x_ref, w_ref, ga_ref, gb_ref, dx_ref, bufa_ref, bufb_ref, r1_ref, r2_ref, r3_ref,
         labown_ref, labrow_ref, lab_ref, m_ref, mt_ref, s_ref, t_ref, scale_ref, srow_ref, st_ref, fin_ref, lossx_ref,
         ag_send, ag_recv, a3_send, a3_recv, lab_send, lab_recv, w_send, w_recv, st_send, st_recv, rs_send, rs_recv,
         hd_send, hd_recv, ls_send, ls_recv, in_sem, p_sem, g_sem, h_sem, out_sem):
    me = lax.axis_index("tp")
    core = lax.rem(me, 2)
    chip = lax.div(me, 2)
    coords = (lax.div(chip, ROWS), lax.rem(lax.div(chip, 4), 4), lax.rem(chip, 4))
    partner = me + 1 - 2 * core

    def ring(axis, d):
        return lax.rem(coords[axis] + d, SIDE)

    def rank(axis, d):
        return me + (ring(axis, d) - coords[axis]) * STRIDES[axis]

    def remote(src, dst, send, recv, target):
        return pltpu.make_async_remote_copy(src_ref=src, dst_ref=dst, send_sem=send, recv_sem=recv,
                                            device_id={"tp": target}, device_id_type=MESH)

    def cols(c):
        return pl.ds(COLOUR * c, COLOUR)

    own = []
    for s in range(SLABS):
        own.append(pltpu.make_async_copy(x_hbm.at[pl.ds(ROWS * s, ROWS)],
                                         x_ref.at[(s,) + coords], in_sem.at[s]))
    own.append(pltpu.make_async_copy(lab_hbm, labown_ref, in_sem.at[2]))
    w_own = pltpu.make_async_copy(w_hbm, w_ref.at[core], in_sem.at[3])
    for copy in own:
        copy.start()
    w_own.start()

    with jax.named_scope("meet"):
        barrier = pltpu.get_barrier_semaphore()
        peers = [partner] + [rank(a, d) for a in range(3) for d in NEXT]
        for peer in peers:
            pl.semaphore_signal(barrier, inc=1, device_id={"tp": peer}, device_id_type=MESH)
        pl.semaphore_wait(barrier, len(peers))

    def ag_copy(s, phase, c, d):
        order = ORDERS[c]
        idx = list(coords)
        for a in order[:phase]:
            idx[a] = ALL
        view = x_ref.at[(s,) + tuple(idx) + (ALL, cols(c))]
        return remote(view, view, ag_send.at[s, phase], ag_recv.at[s, phase],
                      rank(order[phase], d))

    def ag_start(s, phase):
        for d in FAR:
            for c in range(3):
                ag_copy(s, phase, c, d).start()

    def ag_all(s, phase):
        view = (x_ref.at[s, 0, 0, THREE], x_ref.at[s, 0, THREE], x_ref.at[s, THREE])[phase]
        return remote(view, view, ag_send.at[s, phase], ag_recv.at[s, phase], partner)

    def ag_wait(s, phase):
        ag_all(s, phase).wait_recv()

    def near(k):
        return lax.rem(coords[0] + k, SIDE)

    def ag_plane(k, c, d):
        axis = ORDERS[c][2]
        idx = [near(k), ALL, ALL]
        idx[axis] = coords[axis]
        view = x_ref.at[(0,) + tuple(idx) + (ALL, cols(c))]
        return remote(view, view, a3_send.at[0], a3_recv.at[0, k], rank(axis, d))

    def ag_line(k):
        view = x_ref.at[0, coords[0], :, :, :, cols(0)]
        return remote(view, view, a3_send.at[1], a3_recv.at[1, k], rank(0, SIDE - k))

    def ag_near(k):
        for d in FAR:
            for c in (1, 2):
                ag_plane(k, c, d).start()
        if k:
            ag_line(k).start()

    def ag_near_wait(k):
        view = x_ref.at[0, pl.ds(0, 2), 0]
        remote(view, view, a3_send.at[0], a3_recv.at[0, k], partner).wait_recv()

    def ag_line_wait(k):
        view = x_ref.at[0, 0, :, :, :, cols(0)]
        remote(view, view, a3_send.at[1], a3_recv.at[1, k], partner).wait_recv()

    def ag_near_sent():
        view = x_ref.at[0, pl.ds(0, 2)]
        remote(view, view, a3_send.at[0], a3_recv.at[0, 0], partner).wait_send()
        view = x_ref.at[0, THREE, :, :, :, cols(0)]
        remote(view, view, a3_send.at[1], a3_recv.at[1, 0], partner).wait_send()

    def lab_copy(phase, d):
        order = ORDERS[0]
        idx = list(coords)
        for a in order[:phase]:
            idx[a] = ALL
        view = labrow_ref.at[tuple(idx)]
        return remote(view, view, lab_send.at[phase], lab_recv.at[phase], rank(order[phase], d))

    def lab_start(phase):
        for d in NEXT:
            lab_copy(phase, d).start()

    def lab_all(phase):
        view = (labrow_ref.at[0, 0, THREE], labrow_ref.at[0, THREE], labrow_ref.at[THREE])[phase]
        return remote(view, view, lab_send.at[phase], lab_recv.at[phase], partner)

    def lab_wait(phase):
        lab_all(phase).wait_recv()

    with jax.named_scope("ag"):
        for copy in own:
            copy.wait()
        labrow_ref[coords + (ALL, slice(0, SLABS * ROWS))] = labown_ref[...]
        ag_start(0, 0)
        w_copy = remote(w_hbm, w_ref.at[core], w_send, w_recv, partner)
        w_copy.start()
        lab_start(0)
        ag_wait(0, 0)
        ag_start(0, 1)
        ag_start(1, 0)
        lab_wait(0)
        lab_start(1)
        ag_wait(0, 1)
        lab_wait(1)
        lab_start(2)
        ag_near(0)
        ag_near(1)
        ag_wait(1, 0)
        ag_start(1, 1)
        ag_near(2)
        ag_near(3)
        lab_wait(2)

    lane16 = lax.broadcasted_iota(jnp.int32, (ROWS, LANES), 1)
    row16 = lax.broadcasted_iota(jnp.int32, (ROWS, LANES), 0)
    first_col = chip * (2 * HALF)

    def spread(k, carry):
        kz, ky, kx = lax.div(k, ROWS), lax.rem(lax.div(k, 4), 4), lax.rem(k, 4)
        row = jnp.broadcast_to(labrow_ref[kz, ky, kx], (ROWS, LANES)).astype(F32)
        for s in range(SLABS):
            col = jnp.sum(jnp.where(lane16 == row16 + ROWS * s, row, 0.0), axis=1, keepdims=True)
            lab_ref[s, k] = jnp.broadcast_to(col, (ROWS, LANES)).astype(jnp.int32) - first_col - lane16
        return carry

    with jax.named_scope("spread"):
        lax.fori_loop(0, 64, spread, 0, unroll=4)

    bufs = (bufa_ref, bufb_ref)

    def p_copy(n, slot, q, r, rows):
        at = pl.ds(pl.multiple_of(q * BLOCK + r, SUB), rows)
        return pltpu.make_async_copy(bufs[slot].at[at], p_hbm.at[n, at], p_sem.at[slot])

    def p_start(n, slot, r, rows):
        for q in range(4):
            p_copy(n, slot, q, r, rows).start()

    def p_wait(n, slot):
        at = FULL
        pltpu.make_async_copy(bufs[slot].at[at], p_hbm.at[n], p_sem.at[slot]).wait()

    def plane(k):
        return lax.rem(coords[0] + k + 1, SIDE)

    def place(t):
        return lax.div(t, SIDE), plane(lax.rem(t, SIDE))

    def g_load(t, slot):
        s, b = place(t)
        return pltpu.make_async_copy(p_hbm.at[s * SIDE + b], bufs[slot].at[FULL], g_sem.at[slot])

    def p_ahead():
        n = plane(0)

        def line(j, carry):
            q, y, x = lax.div(j, ROWS), lax.rem(lax.div(j, 4), 4), lax.rem(j, 4)
            pltpu.make_async_copy(p_hbm.at[n, pl.ds(pl.multiple_of(j * ROWS, ROWS), ROWS)],
                                  dx_ref.at[1, q, y, x, :, FULL], g_sem.at[2]).start()
            return carry

        lax.fori_loop(0, 64, line, 0)

    def p_there():
        at = FULL
        pltpu.make_async_copy(p_hbm.at[0], bufa_ref.at[at], g_sem.at[2]).wait()

    def st_copy(s, axis, d):
        view = st_ref.at[s, axis, coords[axis]]
        return remote(view, view, st_send.at[s, axis], st_recv.at[s, axis], rank(axis, d))

    def st_all(s, axis):
        view = st_ref.at[s, axis, THREE]
        return remote(view, view, st_send.at[s, axis], st_recv.at[s, axis], partner)

    def st_start(s, axis):
        for d in FAR:
            st_copy(s, axis, d).start()

    def st_merge(s, axis):
        with jax.named_scope("st_wait"):
            st_all(s, axis).wait_recv()
        top = st_ref[s, axis, 0, 0]
        for i in range(1, SIDE):
            top = jnp.maximum(top, st_ref[s, axis, i, 0])
        total = jnp.zeros_like(top)
        target = jnp.zeros_like(top)
        for i in range(SIDE):
            total += st_ref[s, axis, i, 1] * jnp.exp(st_ref[s, axis, i, 0] - top)
            target += st_ref[s, axis, i, 2]
        if axis < 2:
            here = coords[axis + 1]
            st_ref[s, axis + 1, here, 0] = top
            st_ref[s, axis + 1, here, 1] = total
            st_ref[s, axis + 1, here, 2] = target
            st_start(s, axis + 1)
        else:
            fin_ref[s, 0] = top
            fin_ref[s, 1] = INV / total
            fin_ref[s, 2] = top + jnp.log(total) - target

    def z_group(n, slot, i):
        buf = bufs[slot]
        s, b = lax.div(n, SIDE), lax.rem(n, SIDE)
        at = [pl.ds(pl.multiple_of(q * BLOCK + i * SUB, SUB), SUB) for q in range(4)]
        part, row = pl.ds(pl.multiple_of(lax.rem(i, 2) * SUB, SUB), SUB), lax.div(i, 2)
        here = pl.ds(pl.multiple_of(i * SUB, SUB), SUB)
        lab = lab_ref[s, b * ROWS + row, part, :]
        z = [buf[at[q], l * LANES:(l + 1) * LANES] for q in range(4) for l in range(SUB)]
        tops = z
        while len(tops) > 1:
            tops = [jnp.maximum(tops[k], tops[k + 1]) for k in range(0, len(tops), 2)]
        top = tops[0]
        sums = [jnp.zeros((SUB, LANES), F32) for _ in range(2)]
        tgt = [jnp.zeros((SUB, LANES), F32) for _ in range(2)]
        for k in range(32):
            p = jnp.exp(z[k] - top)
            buf[at[k // SUB], k % SUB * LANES:(k % SUB + 1) * LANES] = p
            sums[k % 2] += p
            tgt[k % 2] = jnp.where(lab == k * LANES, z[k], tgt[k % 2])
        mt_ref[here, :] = top
        s_ref[here, :] = sums[0] + sums[1]
        t_ref[here, :] = tgt[0] + tgt[1]

    def z_stat(n):
        s, b = lax.div(n, SIDE), lax.rem(n, SIDE)
        for i in range(2):
            m = mt_ref[i * LANES:(i + 1) * LANES, :]
            m_ref[s, pl.ds(pl.multiple_of(b * BLOCK + i * LANES, LANES), LANES), :] = m
            m_t = m.T
            s_t = s_ref[i * LANES:(i + 1) * LANES, :].T
            t_t = t_ref[i * LANES:(i + 1) * LANES, :].T
            top = jnp.max(m_t, axis=0, keepdims=True)
            at = pl.ds(b * 2 + i, 1)
            srow_ref[0, at, :] = top
            srow_ref[1, at, :] = jnp.sum(s_t * jnp.exp(m_t - top), axis=0, keepdims=True)
            srow_ref[2, at, :] = jnp.sum(t_t, axis=0, keepdims=True)

    def z_step(t, slot):
        s, k = lax.div(t, SIDE), lax.rem(t, SIDE)
        b = near(k)
        n = s * SIDE + b

        @pl.when(t >= 2)
        def _():
            p_wait(n, slot)

        with jax.named_scope("z_dot"):
            xb = x_ref[s, b].reshape(BLOCK, HID)
            for q in range(4):
                bufs[slot][pl.ds(q * BLOCK, BLOCK), :] = jnp.dot(
                    xb, w_ref[q // 2, :, q % 2 * WIDE:(q % 2 + 1) * WIDE], preferred_element_type=F32)
        if slot:
            @pl.when(t == 2 * SIDE - 1)
            def _():
                p_wait(n, 0)
                g_load(1, 0).start()

        def rows(i, carry):
            z_group(n, slot, i)
            return carry

        with jax.named_scope("z_rows"):
            lax.fori_loop(0, 32, rows, 0, unroll=4)
        p_start(n, slot, 0, BLOCK)
        with jax.named_scope("z_stat"):
            z_stat(n)

    def st_begin(s):
        for k in range(3):
            st_ref[s, 0, coords[0], k] = srow_ref[k]
        st_start(s, 0)

    def rs_copy(s, phase, c, d):
        order = ORDERS[c]
        idx = [ALL] * 3
        for a in order[:phase]:
            idx[a] = coords[a]
        idx[order[phase]] = ring(order[phase], d)
        land = (r1_ref, r2_ref, r3_ref)[phase]
        return remote(dx_ref.at[(s,) + tuple(idx) + (ALL, cols(c))], land.at[s, c, d - 1],
                      rs_send.at[s, phase], rs_recv.at[s, phase], rank(order[phase], d))

    def rs_plane(s, k, c, d):
        axis = ORDERS[c][0]
        b = plane(k)
        idx = [b, ALL, ALL]
        if axis:
            idx[axis] = ring(axis, d)
        return remote(dx_ref.at[(s,) + tuple(idx) + (ALL, cols(c))], r1_ref.at[s, c, d - 1, b],
                      rs_send.at[s, 0], rs_recv.at[s, 0], rank(axis, d))

    def rs_line(s, k):
        b = plane(k)
        return remote(dx_ref.at[s, b, :, :, :, cols(2)], r1_ref.at[s, 2, k],
                      rs_send.at[s, 0], rs_recv.at[s, 0], rank(0, k + 1))

    def rs_first(t):
        s, k = lax.div(t, SIDE), lax.rem(t, SIDE)
        for d in FAR:
            for c in range(2):
                rs_plane(s, k, c, d).start()

        @pl.when(k < SIDE - 1)
        def _():
            rs_line(s, k).start()

    def rs_all(s, phase):
        view = (r1_ref.at[s], r2_ref.at[s], r3_ref.at[s])[phase]
        return remote(view, view, rs_send.at[s, phase], rs_recv.at[s, phase], partner)

    def rs_start(s, phase):
        for d in FAR:
            for c in range(3):
                rs_copy(s, phase, c, d).start()

    def rs_add(s, phase):
        with jax.named_scope("rs_wait"):
            rs_all(s, phase).wait_recv()
        for c in range(3):
            order = ORDERS[c]
            sl = slice(c * COLOUR, (c + 1) * COLOUR)
            idx = [None] * 3
            for a in order[:phase + 1]:
                idx[a] = coords[a]
            free = [a for a in range(3) if idx[a] is None]
            if phase == 0:
                def add(i, carry):
                    for j in range(SIDE):
                        at = list(idx)
                        at[free[0]], at[free[1]] = i, j
                        at = (s,) + tuple(at)
                        dx_ref[at + (ALL, sl)] = (
                            (dx_ref[at + (ALL, sl)] + r1_ref[s, c, 0, i, j])
                            + (r1_ref[s, c, 1, i, j] + r1_ref[s, c, 2, i, j]))
                    return carry
                lax.fori_loop(0, SIDE, add, 0)
            elif phase == 1:
                def add(i, carry):
                    at = list(idx)
                    at[free[0]] = i
                    at = (s,) + tuple(at)
                    dx_ref[at + (ALL, sl)] = (
                        (dx_ref[at + (ALL, sl)] + r2_ref[s, c, 0, i])
                        + (r2_ref[s, c, 1, i] + r2_ref[s, c, 2, i]))
                    return carry
                lax.fori_loop(0, SIDE, add, 0)
            else:
                total = ((dx_ref[(s,) + tuple(idx) + (ALL, sl)] + r3_ref[s, c, 0])
                         + (r3_ref[s, c, 1] + r3_ref[s, c, 2]))
                dhid_ref[s * ROWS:(s + 1) * ROWS, sl] = total.astype(BF16)
        if phase < 2:
            rs_start(s, phase + 1)

    gs = (ga_ref, gb_ref)
    last = jnp.int32(2 * SIDE - 1)

    def g_scale(t):
        s, b = place(t)
        for i in range(2):
            at = pl.ds(b * 2 + i, 1)
            top = jnp.broadcast_to(fin_ref[s, 0, at, :], (LANES, LANES)).T
            inv = jnp.broadcast_to(fin_ref[s, 1, at, :], (LANES, LANES)).T
            m = m_ref[s, pl.ds(pl.multiple_of(b * BLOCK + i * LANES, LANES), LANES), :]
            scale_ref[i * LANES:(i + 1) * LANES, :] = jnp.exp(m - top) * inv

    def g_group(t, slot, i, ahead=True):
        s, b = place(t)
        at = [pl.ds(pl.multiple_of(q * BLOCK + i * ROWS, ROWS), ROWS) for q in range(4)]
        here = pl.ds(pl.multiple_of(i * ROWS, ROWS), ROWS)
        lab = lab_ref[s, b * ROWS + i]
        scale = scale_ref[here, :]
        out = pl.ds(pl.multiple_of(lax.div(t, 2) * BLOCK + i * ROWS, ROWS), ROWS)
        for k in range(32):
            lanes = slice(k % SUB * LANES, (k % SUB + 1) * LANES)
            if ahead:
                p = bufs[1 - slot][at[k // SUB], lanes]
            else:
                p = dx_ref[1, k // SUB, lax.div(i, 4), lax.rem(i, 4), :, lanes]
            g = p * scale - jnp.where(lab == k * LANES, INV, 0.0)
            gs[slot][k // ROWS, out, k % ROWS * LANES:(k % ROWS + 1) * LANES] = g.astype(BF16)

    nt = (((1,), (1,)), ((), ()))

    def dx_dot(t, slot, h):
        at = pl.ds(pl.multiple_of(lax.div(t, 2) * BLOCK, BLOCK), BLOCK)
        return lax.dot_general(gs[slot][h, at, :], w_ref[h], nt, preferred_element_type=F32)

    def dx_store(t, dx):
        s, b = place(t)
        dx_ref[s, b] = dx.reshape(SIDE, SIDE, ROWS, HID)

    def g_step(t, slot):
        with jax.named_scope("g_load"):
            g_load(t, 1 - slot).wait()

        @pl.when(t < 2 * SIDE - 1)
        def _():
            pl.when(t == 1)(functools.partial(p_wait, 0, 1))
            g_load(t + 1, slot).start()

        with jax.named_scope("g_step"):
            g_scale(t)
            sb, bb = place(t - 1)

            def part(h, carry):
                dx = dx_dot(t - 1, 1 - slot, h).reshape(SIDE, SIDE, ROWS, HID)
                for i in range(SUB):
                    g_group(t, slot, h * SUB + i)
                dx_ref[sb, bb] = dx + jnp.where(h == 0, 0.0, dx_ref[sb, bb])
                return carry

            lax.fori_loop(0, 2, part, 0)

    with jax.named_scope("first_wait"):
        w_own.wait()
        w_copy.wait_recv()
        ag_near_wait(0)

    def z_pair(i, carry):
        t = 2 * i

        with jax.named_scope("z_wait"):
            @pl.when(i == 1)
            def _():
                ag_near_wait(2)
                ag_line_wait(2)

            pl.when(i == 2)(functools.partial(ag_wait, 1, 2))
        z_step(t, 0)
        with jax.named_scope("z_wait"):
            @pl.when(i == 0)
            def _():
                ag_wait(1, 1)
                ag_start(1, 2)
                ag_near_wait(1)
                ag_line_wait(1)

            @pl.when(i == 1)
            def _():
                ag_near_wait(3)
                ag_line_wait(3)

            pl.when(i == 2)(functools.partial(st_merge, 0, 0))
            pl.when(i == 3)(functools.partial(st_merge, 0, 2))
        z_step(t + 1, 1)

        @pl.when(i == 1)
        def _():
            st_begin(0)
            p_ahead()

        pl.when(i == 2)(functools.partial(st_merge, 0, 1))
        return carry

    lax.fori_loop(0, SIDE, z_pair, 0)
    st_begin(1)

    def g_first(i, carry):
        g_group(jnp.int32(0), 0, i, False)
        return carry

    with jax.named_scope("g_first"):
        g_scale(jnp.int32(0))
        p_there()
        lax.fori_loop(0, ROWS, g_first, 0, unroll=2)

    def g_pair(i, carry):
        t = 2 * i + 1
        g_step(t, 1)
        pl.when(i == 0)(functools.partial(st_merge, 1, 0))
        pl.when(i == 1)(functools.partial(st_merge, 1, 2))
        rs_first(t - 1)

        @pl.when(i < SIDE - 1)
        def _():
            g_step(t + 1, 0)
            pl.when(i == 0)(functools.partial(st_merge, 1, 1))
            rs_first(t)

        return carry

    lax.fori_loop(0, SIDE, g_pair, 0)
    with jax.named_scope("dx_last"):
        dx_store(last, dx_dot(last, 1, 0) + dx_dot(last, 1, 1))
    rs_first(last)
    rs_add(0, 0)

    lossx_ref[core] = fin_ref[0, 2] + fin_ref[1, 2]
    ls_copy = remote(lossx_ref.at[core], lossx_ref.at[core], ls_send, ls_recv, partner)
    ls_copy.start()

    ls_copy.wait_recv()
    loss_ref[0] = jnp.sum(lossx_ref[0] + lossx_ref[1]) * INV

    def flip(j, carry):
        t, part = lax.div(j, 2), lax.rem(j, 2)
        s, b = place(t)
        xs = x_ref[s, b, pl.ds(part * 2, 2)].reshape(LANES, HID)
        at = lax.rem(t, 2) * WIDE + lax.div(t, 2) * BLOCK + part * LANES
        w_ref[1, :, pl.ds(pl.multiple_of(at, LANES), LANES)] = xs.T
        return carry

    with jax.named_scope("flip"):
        lax.fori_loop(0, 2 * WIDE // LANES, flip, 0)

    def half(slot):
        return pl.ds(pl.multiple_of(slot * HEAD, HEAD), HEAD)

    def head_copy(j):
        slot = lax.rem(j, 2)
        return remote(bufa_ref.at[:, half(slot)], hrecv_hbm.at[j], hd_send.at[slot], hd_recv.at[j], partner)

    def head_load(j):
        return pltpu.make_async_copy(hrecv_hbm.at[j], bufb_ref.at[:, pl.ds(HEAD, HEAD)], h_sem)

    def head_dot(h, j, buf, at):
        with jax.named_scope("h_dot"):
            for r in range(0, HID, HEAD_ROWS):
                r = pl.ds(r, HEAD_ROWS)
                buf[r, at] = (jnp.dot(w_ref[1, r, :WIDE], ga_ref[h, :, half(j)], preferred_element_type=F32)
                              + jnp.dot(w_ref[1, r, WIDE:], gb_ref[h, :, half(j)], preferred_element_type=F32))

    def out_copy(j):
        return pltpu.make_async_copy(w_ref.at[0, :, half(j)], dhead_hbm.at[:, half(j)], out_sem.at[j])

    def theirs(j):
        @pl.when(jnp.int32(j) >= 2)
        def _():
            head_copy(j - 2).wait_send()

        head_dot(1 - core, j, bufa_ref, half(lax.rem(j, 2)))
        head_copy(j).start()

    def ours(j):
        head_dot(core, j, bufb_ref, pl.ds(0, HEAD))

    def fetch(j):
        with jax.named_scope("h_wait"):
            head_copy(j).wait_recv()
        head_load(j).start()

    def finish(j):
        with jax.named_scope("h_load"):
            head_load(j).wait()

        def add(i, carry):
            r = pl.ds(pl.multiple_of(i * ROWS, ROWS), ROWS)
            w_ref[0, r, half(j)] = (bufb_ref[r, pl.ds(0, HEAD)] + bufb_ref[r, pl.ds(HEAD, HEAD)]).astype(BF16)
            return carry

        with jax.named_scope("h_add"):
            lax.fori_loop(0, HID // ROWS, add, 0, unroll=SIDE)
        out_copy(j).start()

    def pair(r, carry):
        theirs(r + 1)

        @pl.when(r > 0)
        def _():
            finish(r - 1)

        pl.when(r == 1)(functools.partial(rs_add, 0, 1))
        ours(r)
        fetch(r)
        pl.when(r == 0)(functools.partial(rs_add, 1, 0))
        pl.when(r == 2)(functools.partial(rs_add, 1, 1))
        return carry

    theirs(0)
    lax.fori_loop(0, 3, pair, 0)
    rs_add(0, 2)
    finish(2)
    fetch(3)
    ours(3)
    finish(3)
    rs_add(1, 2)
    head_copy(2).wait_send()
    head_copy(3).wait_send()

    with jax.named_scope("tail"):
        for j in range(4):
            out_copy(j).wait()
        w_copy.wait_send()
        ls_copy.wait_send()
        ag_near_sent()
        for phase in range(3):
            lab_all(phase).wait_send()
            for s in range(SLABS):
                st_all(s, phase).wait_send()
                if s or phase < 2:
                    ag_all(s, phase).wait_send()
                rs_all(s, phase).wait_send()


PIECES = 8


def hand_out(loss_in, dhid_in, dhead_in, loss_out, dhid_out, dhead_out, dhid_v, dhead_v, in_sem, out_sem):
    ways = [(dhid_in, dhid_v, dhid_out)]
    for i in range(PIECES):
        at = pl.ds(i * (HID // PIECES), HID // PIECES)
        ways.append((dhead_in.at[at], dhead_v.at[at], dhead_out.at[at]))
    ins = [pltpu.make_async_copy(a, v, in_sem.at[i]) for i, (a, v, _) in enumerate(ways)]
    outs = [pltpu.make_async_copy(v, o, out_sem.at[i]) for i, (_, v, o) in enumerate(ways)]
    for copy in ins:
        copy.start()
    loss_out[0] = loss_in[0]
    for here, there in zip(ins, outs):
        here.wait()
        there.start()
    for copy in outs:
        copy.wait()


def solution(mesh):
    any_space = pl.BlockSpec(memory_space=pl.ANY)
    vmem = pl.BlockSpec(memory_space=pltpu.VMEM)
    smem = pl.BlockSpec(memory_space=pltpu.SMEM)
    dma = pltpu.SemaphoreType.DMA

    def local_step(hid_loc, w_loc, lab_loc):
        labels = lab_loc.reshape(1, -1)
        flops = 3 * 2 * TOKENS * HID * HALF
        loss, d_hidden, d_head, _, _ = pl.pallas_call(
            body,
            out_shape=(
                jax.ShapeDtypeStruct((1,), F32),
                jax.ShapeDtypeStruct((SLABS * ROWS, HID), BF16),
                jax.ShapeDtypeStruct((HID, HALF), BF16),
                jax.ShapeDtypeStruct((SUB, WIDE, WIDE), F32),
                jax.ShapeDtypeStruct((4, HID, HEAD), F32),
            ),
            in_specs=[any_space, any_space, any_space],
            out_specs=(smem, vmem, any_space, any_space, any_space),
            scratch_shapes=[
                pltpu.VMEM((SLABS, SIDE, SIDE, SIDE, ROWS, HID), BF16),
                pltpu.VMEM((2, HID, HALF), BF16),
                pltpu.VMEM((2, WIDE, HALF), BF16),
                pltpu.VMEM((2, WIDE, HALF), BF16),
                pltpu.VMEM((SLABS, SIDE, SIDE, SIDE, ROWS, HID), F32),
                pltpu.VMEM((HID, WIDE), F32),
                pltpu.VMEM((HID, WIDE), F32),
                pltpu.VMEM((SLABS, 3, 3, SIDE, SIDE, ROWS, COLOUR), F32),
                pltpu.VMEM((SLABS, 3, 3, SIDE, ROWS, COLOUR), F32),
                pltpu.VMEM((SLABS, 3, 3, ROWS, COLOUR), F32),
                pltpu.VMEM((1, SLABS * ROWS), jnp.int32),
                pltpu.VMEM((SIDE, SIDE, SIDE, 1, LANES), jnp.int32),
                pltpu.VMEM((SLABS, 64, ROWS, LANES), jnp.int32),
                pltpu.VMEM((SLABS, WIDE, LANES), F32),
                pltpu.VMEM((BLOCK, LANES), F32),
                pltpu.VMEM((BLOCK, LANES), F32),
                pltpu.VMEM((BLOCK, LANES), F32),
                pltpu.VMEM((BLOCK, LANES), F32),
                pltpu.VMEM((3, SUB, LANES), F32),
                pltpu.VMEM((SLABS, 3, SIDE, 3, SUB, LANES), F32),
                pltpu.VMEM((SLABS, 3, SUB, LANES), F32),
                pltpu.VMEM((2, SUB, LANES), F32),
                dma((SLABS, 3)), dma((SLABS, 3)), dma((2,)), dma((2, SIDE)),
                dma((3,)), dma((3,)),
                dma, dma,
                dma((SLABS, 3)), dma((SLABS, 3)),
                dma((SLABS, 3)), dma((SLABS, 3)),
                dma((2,)), dma((4,)),
                dma, dma,
                dma((4,)), dma((2,)), dma((3,)), dma, dma((4,)),
            ],
            compiler_params=pltpu.CompilerParams(
                collective_id=0, has_side_effects=True, vmem_limit_bytes=67043328),
            cost_estimate=pl.CostEstimate(flops=flops, bytes_accessed=100_000_000, transcendentals=TOKENS * HALF),
        )(hid_loc, w_loc, labels)
        return pl.pallas_call(
            hand_out,
            out_shape=(
                jax.ShapeDtypeStruct((1,), F32),
                jax.ShapeDtypeStruct((SLABS * ROWS, HID), BF16),
                jax.ShapeDtypeStruct((HID, HALF), BF16),
            ),
            in_specs=[smem, any_space, any_space],
            out_specs=(smem, any_space, any_space),
            scratch_shapes=[
                pltpu.VMEM((SLABS * ROWS, HID), BF16),
                pltpu.VMEM((HID, HALF), BF16),
                dma((PIECES + 1,)), dma((PIECES + 1,)),
            ],
        )(loss, d_hidden, d_head)

    return jax.shard_map(
        local_step,
        mesh=mesh,
        in_specs=(P(("dp", "tp"), None), P(None, "tp"), P(("dp", "tp"))),
        out_specs=(P("dp"), P(("dp", "tp"), None), P("dp", "tp")),
        check_vma=False,
    )
```
